32 devices in a mesh: grp: 4 (over y, x), dev: 8 (over z, core).
Axes of the slice: x: 2, y: 2, z: 4, core: 2. Of those that a mesh axis runs over, the one named last changes fastest.
Arguments:
- token_ids: int32 [128, 128], P(('grp', 'dev')), may hold values from 0 to 128255, as said below
- sensitivity: bfloat16 [128, 128, 4096], P(('grp', 'dev')), may hold values from -6 to 6
- last_hidden: bfloat16 [128, 4096], P(('grp', 'dev')), may hold values from -6 to 6
- lengths: int32 [128], P(('grp', 'dev')), may hold values from 97 to 128
- norm_gain: float32 [4096], replicated, may hold values from 0.25 to 1.75
- reward_head: float32 [4096], replicated, may hold values from -0.09375 to 0.09375
- chosen_index: int32 [64], replicated, may hold values from 0 to 127, as said below
- rejected_index: int32 [64], replicated, may hold values from 0 to 127, as said below
- shard_owner: int32 [32], replicated, may hold values from 0 to 31, each once
Outputs:
- owned_grad: bfloat16 [128256, 4096], P(('grp', 'dev'))
- head_grad: float32 [4096], P(('grp', 'dev'))
The draws below stay inside these ranges and needn't reach their ends.
Inputs may be any that keep to these rules, and one draw needn't show every extreme that they name: `token_ids`: within the token slots of one device, at most 32 ids fall in any one vocabulary shard of 4008 rows, and on every device some shard gets exactly 32. chosen_index and rejected_index together name every response exactly once. `rejected_index`: see chosen_index.
All inputs are finite; a program needn't handle non-finite values.
Results may differ from the reference program's by a relative error of at most 0.0042.
Values may be sent and summed in bfloat16 or wider, within the bound.
A program may use at most 128 MiB of HBM per device.

```python
import jax
import jax.numpy as jnp
from jax import lax

D = 4096
VOCAB = 128256
BLOCK = 128
RESP_DEV = 4
TOK_DEV = 512
RESPONSES = 128
PAIRS = 64
SHARD = 4008
CAP = 32
DEVICES = 32


def pair_split(key):
    order = jax.random.permutation(jax.random.fold_in(key, 7), RESPONSES).astype(jnp.int32)
    return (order[:PAIRS], order[PAIRS:])


def draw_chosen_index(key, part):
    return pair_split(key)[0]


def draw_rejected_index(key, part):
    return pair_split(key)[1]


def draw_token_ids(key, part):
    total = DEVICES * CAP

    def one_device(dev_key):
        key_first, key_order, key_shuffle, key_offset = jax.random.split(dev_key, 4)
        labels = jnp.arange(total, dtype=jnp.int32) // CAP
        within = jnp.arange(total, dtype=jnp.int32) % CAP
        first = jax.random.randint(key_first, (), 0, DEVICES, dtype=jnp.int32)
        order = jax.random.permutation(key_order, total).astype(jnp.int32)
        score = jnp.where(labels == first, within - CAP, order)
        picked = jnp.argsort(score, stable=True)[:TOK_DEV]
        shards = jax.random.permutation(key_shuffle, labels[picked])
        offset = jax.random.randint(key_offset, (TOK_DEV,), 0, SHARD, dtype=jnp.int32)
        return (shards * SHARD + offset).astype(jnp.int32)
    keys = jax.random.split(jax.random.fold_in(key, 11), DEVICES)
    return jax.vmap(one_device)(keys).reshape(RESPONSES, BLOCK)


def set_ends(drawn, stream_key, low, top_value):
    longest = drawn.shape.index(max(drawn.shape))
    spots = []
    for shift in (0, 1):
        where = [jax.random.randint(jax.random.fold_in(stream_key, axis), (), 0, length) for axis, length in enumerate(drawn.shape)]
        where[longest] = (where[longest] + shift) % drawn.shape[longest]
        spots.append(tuple(where))
    return drawn.at[spots[0]].set(low).at[spots[1]].set(top_value)


def level_of(own_key, extent, cuts, smallest, largest):
    loudness = 1.0
    for axis_at, parts in cuts:
        draws = jax.random.uniform(jax.random.fold_in(jax.random.fold_in(own_key, 6), axis_at), (parts,), jnp.float32, smallest / len(cuts), largest / len(cuts))
        loudness = loudness * jnp.repeat(jnp.exp(draws), extent[axis_at] // parts).reshape((-1,) + (1,) * (len(extent) - 1 - axis_at))
    return loudness


def normal_values(rng, dims, width, limit, cuts=(), held_as=jnp.bfloat16):
    result = jax.random.normal(rng, dims, jnp.float32) * width
    if len(cuts) > 0:
        result = level_of(rng, dims, cuts, -0.22, 0.18) * result
    return jnp.clip(result, min=-limit, max=limit).astype(held_as)


def setup_inputs(seed: int = 0) -> dict:
    arg_keys = jax.random.split(jax.random.key(seed), 10)
    token_ids = draw_token_ids(jax.random.fold_in(arg_keys[9], 71), 0)
    sensitivity = normal_values(arg_keys[1], (RESPONSES, BLOCK, D), 1.0, 6.0, ((0, 32),))
    last_hidden = normal_values(arg_keys[2], (RESPONSES, D), 1.0, 6.0, ((0, 32),))
    lengths = set_ends(jax.random.randint(arg_keys[3], (RESPONSES,), BLOCK - BLOCK // 4 + 1, BLOCK + 1), jax.random.fold_in(arg_keys[3], 1), BLOCK - BLOCK // 4 + 1, BLOCK).astype(jnp.int32)
    norm_gain = jnp.clip(1.0 + 0.15 * jax.random.normal(arg_keys[4], (D,), jnp.float32), 0.25, 1.75)
    reward_head = normal_values(arg_keys[5], (D,), D ** -0.5, 0.09375, (), jnp.float32)
    chosen_index = draw_chosen_index(jax.random.fold_in(arg_keys[9], 71), 0)
    rejected_index = draw_rejected_index(jax.random.fold_in(arg_keys[9], 71), 0)
    shard_owner = jax.random.permutation(arg_keys[8], DEVICES).astype(jnp.int32)
    return {"token_ids": token_ids, "sensitivity": sensitivity, "last_hidden": last_hidden, "lengths": lengths, "norm_gain": norm_gain, "reward_head": reward_head, "chosen_index": chosen_index, "rejected_index": rejected_index, "shard_owner": shard_owner}


def reference(token_ids, sensitivity, last_hidden, lengths, norm_gain, reward_head, chosen_index, rejected_index, shard_owner):
    hidden = last_hidden.astype(jnp.float32)
    normed = hidden / jnp.sqrt(lax.optimization_barrier(jnp.mean(hidden * hidden, axis=-1, keepdims=True)) + 1e-05) * norm_gain
    reward = lax.optimization_barrier(jnp.sum(normed * reward_head, axis=-1))
    margin = reward[chosen_index] - reward[rejected_index]
    push = -jax.nn.sigmoid(-margin)
    reward_grad = jnp.zeros((RESPONSES,), jnp.float32).at[chosen_index].add(push).at[rejected_index].add(-push)
    head_grad = lax.optimization_barrier(jnp.sum(reward_grad[:, None] * normed, axis=0))
    slots = jnp.arange(BLOCK, dtype=jnp.int32)
    live = slots[None, :] < lengths[:, None]
    scale_all = jnp.where(live, reward_grad[:, None], jnp.float32(0.0))
    ids_dev = token_ids.reshape(DEVICES, RESP_DEV * BLOCK)
    sens_dev = sensitivity.reshape(DEVICES, RESP_DEV * BLOCK, D)
    scale_dev = scale_all.reshape(DEVICES, RESP_DEV * BLOCK)

    def accumulate(table, items):
        ids, sens, scale = items
        rows = (scale[:, None] * sens.astype(jnp.float32)).astype(jnp.bfloat16)
        return (table.at[ids].add(rows.astype(jnp.float32)), None)
    table = jnp.zeros((VOCAB, D), jnp.float32)
    table, _ = lax.scan(accumulate, table, (ids_dev, sens_dev, scale_dev))
    inverse = jnp.argsort(shard_owner).astype(jnp.int32)
    owned = table.reshape(DEVICES, SHARD, D)[inverse].reshape(VOCAB, D)
    return (owned.astype(jnp.bfloat16), head_grad)
```

```python
import functools

import jax
import jax.numpy as jnp
from jax import lax
from jax.experimental import pallas as pl
from jax.experimental.pallas import tpu as pltpu
from jax.sharding import PartitionSpec as P

VOCAB = 128256
MESH = pl.DeviceIdType.MESH


def exchange_kernel(n, n_dev, meta_ref, rows_ref, meta_out, rows_out, send_sem, recv_sem, own_sem):
    me = lax.axis_index("grp") * n_dev + lax.axis_index("dev")

    def coord(t):
        return (t // n_dev, lax.rem(t, n_dev))

    barrier = pltpu.get_barrier_semaphore()

    def greet(k, c):
        t = lax.rem(me + k, n)
        pl.semaphore_signal(barrier, inc=1, device_id=coord(t), device_id_type=MESH)
        return c

    lax.fori_loop(1, n, greet, 0)
    own = [
        pltpu.make_async_copy(src.at[me], dst.at[me], own_sem.at[i])
        for i, (src, dst) in enumerate(((meta_ref, meta_out), (rows_ref, rows_out)))
    ]
    for c in own:
        c.start()
    pl.semaphore_wait(barrier, n - 1)

    def copies(src_block, dst_block, to):
        return [
            pltpu.make_async_remote_copy(
                src_ref=src.at[src_block],
                dst_ref=dst.at[dst_block],
                send_sem=send_sem.at[i, src_block],
                recv_sem=recv_sem.at[i, dst_block],
                device_id=coord(to),
                device_id_type=MESH,
            )
            for i, (src, dst) in enumerate(((meta_ref, meta_out), (rows_ref, rows_out)))
        ]

    def send(k, c):
        t = lax.rem(me + k, n)
        for cp in copies(t, me, t):
            cp.start()
        return c

    lax.fori_loop(1, n, send, 0)

    def finish(k, c):
        t = lax.rem(me + k, n)
        for cp in copies(t, me, t):
            cp.wait_send()
        s = lax.rem(me + n - k, n)
        for cp in copies(s, s, s):
            cp.wait_recv()
        return c

    lax.fori_loop(1, n, finish, 0)
    for c in own:
        c.wait()


def exchange(meta, rows, n, n_dev):
    anyspec = pl.BlockSpec(memory_space=pl.ANY)
    return pl.pallas_call(
        functools.partial(exchange_kernel, n, n_dev),
        out_shape=(
            jax.ShapeDtypeStruct(meta.shape, meta.dtype),
            jax.ShapeDtypeStruct(rows.shape, rows.dtype),
        ),
        in_specs=[anyspec, anyspec],
        out_specs=(anyspec, anyspec),
        scratch_shapes=[
            pltpu.SemaphoreType.DMA((2, n)),
            pltpu.SemaphoreType.DMA((2, n)),
            pltpu.SemaphoreType.DMA((2,)),
        ],
        compiler_params=pltpu.CompilerParams(collective_id=1, has_side_effects=True),
    )(meta, rows)


GROUP = 8
NEAR = 32
FAR = 16
FWD = 8


def relay_kernel(n_grp, n_dev, fm_ref, slots_ref, pmeta_ref, fm_out, rows_out, fmeta_out,
                 pin, pmeta_in, fwd, fwd_meta, fm_sems, near_sems, far_sems, piece_sems,
                 pm_sems, fwd_sems, fwdm_sems, own_sems):
    g = lax.axis_index("grp")
    v = lax.axis_index("dev")
    hd = n_dev // 2
    local_n = n_grp * hd
    half = v // hd
    u = lax.rem(v, hd)
    me = g * n_dev + v
    me_local = g * hd + u
    n = n_grp * n_dev
    pieces = n_grp + 1
    near_g, far_g = NEAR // GROUP, FAR // GROUP
    far_base = local_n * near_g
    piece_base = far_base + local_n * far_g
    fwd_base = piece_base
    other = 1 - half

    def coord(t):
        return (t // n_dev, lax.rem(t, n_dev))

    barrier = pltpu.get_barrier_semaphore()

    def greet(k, c):
        pl.semaphore_signal(
            barrier, inc=1, device_id=coord(lax.rem(me + k, n)), device_id_type=MESH
        )
        return c

    lax.fori_loop(1, n, greet, 0)

    def local_copy(src, dst, i):
        return pltpu.make_async_copy(src, dst, own_sems.at[i])

    own = [
        local_copy(fm_ref.at[me], fm_out.at[me], 0),
        local_copy(
            slots_ref.at[pl.ds(me_local * near_g, near_g)],
            rows_out.at[pl.ds(me_local * near_g, near_g)],
            1,
        ),
    ]
    for cp in own:
        cp.start()
    pl.semaphore_wait(barrier, n - 1)

    def remote(src, dst, send_sem, recv_sem, to):
        return pltpu.make_async_remote_copy(
            src_ref=src,
            dst_ref=dst,
            send_sem=send_sem,
            recv_sem=recv_sem,
            device_id=to,
            device_id_type=MESH,
        )

    def piece_target(q):
        if q < n_grp:
            return (lax.rem(g + q, n_grp), other * hd + u)
        return (g, other * hd + lax.rem(u + hd // 2, hd))

    piece_copies = []
    for q in range(pieces):
        to = piece_target(q)
        piece_copies.append(
            remote(slots_ref.at[piece_base + q], pin.at[q],
                   piece_sems.at[0, q], piece_sems.at[1, q], to)
        )
        piece_copies.append(
            remote(pmeta_ref.at[q], pmeta_in.at[q], pm_sems.at[0, q], pm_sems.at[1, q], to)
        )
    for cp in piece_copies:
        cp.start()

    def fm_copy(src, dst, k):
        return remote(fm_ref.at[src], fm_out.at[dst], fm_sems.at[0, k], fm_sems.at[1, k],
                      coord(src))

    def split(k):
        a = k // hd
        b = lax.rem(k, hd)
        return a, b

    def near_copy(k):
        a, b = split(k)
        tg, tu = lax.rem(g + a, n_grp), lax.rem(u + b, hd)
        t = tg * hd + tu
        return remote(
            slots_ref.at[pl.ds(t * near_g, near_g)],
            rows_out.at[pl.ds(me_local * near_g, near_g)],
            near_sems.at[0, k],
            near_sems.at[1, k],
            (tg, half * hd + tu),
        )

    def far_copy(k):
        a, b = split(k)
        tg, tu = lax.rem(g + a, n_grp), lax.rem(u + b, hd)
        t = tg * hd + tu
        return remote(
            slots_ref.at[pl.ds(far_base + t * far_g, far_g)],
            rows_out.at[pl.ds(far_base + me_local * far_g, far_g)],
            far_sems.at[0, k],
            far_sems.at[1, k],
            (tg, other * hd + tu),
        )

    def send_fm(k, c):
        fm_copy(lax.rem(me + k, n), me, k).start()
        return c

    lax.fori_loop(1, n, send_fm, 0)

    def send_far(k, c):
        far_copy(k).start()
        return c

    def send_near(k, c):
        near_copy(k).start()
        return c

    lax.fori_loop(0, local_n, send_far, 0)

    for cp in piece_copies:
        cp.wait_recv()
    count = pieces * GROUP
    marks = pmeta_in[...].reshape(count, 128)
    used = marks[:, 0:1] > 0.0
    dst = (marks[:, 1:2] * hd + marks[:, 2:3]).astype(jnp.int32)
    lane = lax.broadcasted_iota(jnp.int32, (count, 128), 1)
    hot = jnp.where((lane == dst) & used, 1.0, 0.0)
    row_i = lax.broadcasted_iota(jnp.int32, (count, count), 0)
    col_i = lax.broadcasted_iota(jnp.int32, (count, count), 1)
    earlier = jnp.where(row_i > col_i, 1.0, 0.0)
    before = jnp.dot(earlier, hot, preferred_element_type=jnp.float32)
    rank = jnp.sum(before * hot, axis=1, keepdims=True).astype(jnp.int32)
    slot = jnp.where(used & (rank < FWD), dst * FWD + rank, -1)
    place = jnp.where(lane == slot, 1.0, 0.0)
    contract = (((0,), (0,)), ((), ()))
    width = pin.shape[2]
    chunk = 512

    def gather(c, carry):
        cols = pl.ds(pl.multiple_of(c * chunk, chunk), chunk)
        rows = pin[:, :, cols].astype(jnp.float32).reshape(count, chunk)
        out = lax.dot_general(place, rows, contract, preferred_element_type=jnp.float32)
        fwd[:, :, cols] = out.reshape(local_n, FWD, chunk).astype(jnp.bfloat16)
        return carry

    lax.fori_loop(0, width // chunk, gather, 0)
    fwd_meta[...] = lax.dot_general(
        place, marks, contract, preferred_element_type=jnp.float32
    ).reshape(local_n, FWD, 128)

    def fwd_copies(k):
        a, b = split(k)
        tg, tu = lax.rem(g + a, n_grp), lax.rem(u + b, hd)
        t = tg * hd + tu
        to = (tg, half * hd + tu)
        return [
            remote(fwd.at[t], rows_out.at[fwd_base + me_local],
                   fwd_sems.at[0, k], fwd_sems.at[1, k], to),
            remote(fwd_meta.at[t], fmeta_out.at[me_local],
                   fwdm_sems.at[0, k], fwdm_sems.at[1, k], to),
        ]

    own_fwd = [
        local_copy(fwd.at[me_local], rows_out.at[fwd_base + me_local], 2),
        local_copy(fwd_meta.at[me_local], fmeta_out.at[me_local], 3),
    ]
    for cp in own_fwd:
        cp.start()

    def send_fwd(k, c):
        for cp in fwd_copies(k):
            cp.start()
        return c

    lax.fori_loop(1, local_n, send_fwd, 0)
    lax.fori_loop(1, local_n, send_near, 0)

    for cp in piece_copies:
        cp.wait_send()

    def finish_far(k, c):
        cp = far_copy(k)
        cp.wait_send()
        cp.wait_recv()
        return c

    def finish_near(k, c):
        for cp in [near_copy(k)] + fwd_copies(k):
            cp.wait_send()
            cp.wait_recv()
        return c

    def finish_fm(k, c):
        cp = fm_copy(lax.rem(me + k, n), me, k)
        cp.wait_send()
        cp.wait_recv()
        return c

    lax.fori_loop(1, n, finish_fm, 0)
    lax.fori_loop(0, local_n, finish_far, 0)
    lax.fori_loop(1, local_n, finish_near, 0)
    for cp in own + own_fwd:
        cp.wait()


def relay_exchange(fm, slots, pmeta, n_grp, n_dev):
    n = n_grp * n_dev
    local_n = n // 2
    width = slots.shape[2]
    pieces = n_grp + 1
    groups = local_n * (NEAR + FAR + FWD) // GROUP
    anyspec = pl.BlockSpec(memory_space=pl.ANY)
    sem = pltpu.SemaphoreType.DMA
    return pl.pallas_call(
        functools.partial(relay_kernel, n_grp, n_dev),
        out_shape=(
            jax.ShapeDtypeStruct(fm.shape, fm.dtype),
            jax.ShapeDtypeStruct((groups, GROUP, width), slots.dtype),
            jax.ShapeDtypeStruct((local_n, FWD, 128), jnp.float32),
        ),
        in_specs=[anyspec, anyspec, anyspec],
        out_specs=(anyspec, anyspec, anyspec),
        scratch_shapes=[
            pltpu.VMEM((pieces, GROUP, width), slots.dtype),
            pltpu.VMEM((pieces, GROUP, 128), jnp.float32),
            pltpu.VMEM((local_n, FWD, width), slots.dtype),
            pltpu.VMEM((local_n, FWD, 128), jnp.float32),
            sem((2, n)),
            sem((2, local_n)),
            sem((2, local_n)),
            sem((2, pieces)),
            sem((2, pieces)),
            sem((2, local_n)),
            sem((2, local_n)),
            sem((4,)),
        ],
        compiler_params=pltpu.CompilerParams(collective_id=0, has_side_effects=True),
    )(fm, slots, pmeta)


def local(token_ids, sensitivity, last_hidden, lengths, norm_gain, reward_head,
          chosen_index, rejected_index, shard_owner):
    args = (token_ids, sensitivity, last_hidden, lengths, norm_gain, reward_head,
            chosen_index, rejected_index, shard_owner)
    resp_local, block_len = token_ids.shape
    devices = shard_owner.shape[0]
    n_grp, n_dev = lax.axis_size("grp"), lax.axis_size("dev")
    capacity = max(2, (2 * resp_local * block_len + devices - 1) // devices)
    if (capacity == NEAR and n_dev % 4 == 0 and devices * resp_local <= 128
            and resp_local <= 4 and devices // 2 * FWD <= 128
            and VOCAB // devices < 64 * 250):
        return relay_local(*args)
    prep = prepare(*args)
    return plain_finish(prep, n_dev)


def prepare(token_ids, sensitivity, last_hidden, lengths, norm_gain, reward_head,
            chosen_index, rejected_index, shard_owner):
    resp_local, block_len = token_ids.shape
    width = sensitivity.shape[2]
    tok_local = resp_local * block_len
    devices = shard_owner.shape[0]
    shard_rows = VOCAB // devices
    capacity = max(2, (2 * tok_local + devices - 1) // devices)
    hidden = last_hidden.astype(jnp.float32)
    normed = (
        hidden / jnp.sqrt(jnp.mean(hidden * hidden, axis=-1, keepdims=True) + 1e-05) * norm_gain
    )
    own_reward = jnp.sum(normed * reward_head, axis=-1)

    positions = jnp.arange(block_len, dtype=jnp.int32)
    live = (positions[None, :] < lengths[:, None]).reshape(tok_local)
    ids = token_ids.reshape(tok_local)
    shard_of = ids // shard_rows
    offset = ids - shard_of * shard_rows
    shard_hot = shard_of[:, None] == jnp.arange(devices, dtype=jnp.int32)[None, :]
    owner = jnp.sum(jnp.where(shard_hot, shard_owner[None, :], 0), axis=1)
    owner_hot = (owner[:, None] == jnp.arange(devices, dtype=jnp.int32)[None, :]) & live[:, None]
    live_hot = owner_hot.astype(jnp.bfloat16)
    token_pos = jnp.arange(tok_local, dtype=jnp.int32)
    earlier = (token_pos[:, None] > token_pos[None, :]).astype(jnp.bfloat16)
    before = jnp.dot(earlier, live_hot, preferred_element_type=jnp.float32)
    rank = jnp.sum(before * live_hot.astype(jnp.float32), axis=1).astype(jnp.int32)
    counts = jnp.sum(owner_hot.astype(jnp.int32), axis=0)
    return dict(
        sens=sensitivity.reshape(tok_local, width), normed=normed, own_reward=own_reward,
        live=live, offset=offset, owner=owner, rank=rank, counts=counts,
        owner_hot=owner_hot, resp=token_pos // block_len, capacity=capacity,
        chosen_index=chosen_index, rejected_index=rejected_index, devices=devices,
        shard_rows=shard_rows, resp_local=resp_local, width=width, tok_local=tok_local,
    )


def lane_pad(a, lanes):
    return jnp.pad(a, ((0, 0), (0, lanes - a.shape[1])))[:, None, :]


def reward_grads(p, reward):
    responses = p["devices"] * p["resp_local"]
    all_resp = jnp.arange(responses, dtype=jnp.int32)
    sign_table = (p["chosen_index"][:, None] == all_resp[None, :]).astype(jnp.float32) - (
        p["rejected_index"][:, None] == all_resp[None, :]
    ).astype(jnp.float32)
    margin = jnp.sum(sign_table * reward[None, :], axis=1)
    push = -jax.nn.sigmoid(-margin)
    return jnp.sum(sign_table * push[:, None], axis=0)


def place_all(shard_rows, rows, targets, scale):
    scaled = (scale[:, None] * rows).astype(jnp.bfloat16)
    placing = (targets[None, :] == jnp.arange(shard_rows, dtype=jnp.int32)[:, None]).astype(
        jnp.bfloat16
    )
    return jnp.dot(placing, scaled, preferred_element_type=jnp.float32).astype(jnp.bfloat16)


def plain_finish(p, n_dev):
    devices, capacity, resp_local = p["devices"], p["capacity"], p["resp_local"]
    width = p["width"]
    cols = width // devices
    responses = devices * resp_local
    lanes = -(-max(cols, capacity, resp_local) // 128) * 128
    slot = jnp.where(p["live"], p["owner"] * capacity + p["rank"], -1)
    slot_match = slot[None, :] == jnp.arange(devices * capacity, dtype=jnp.int32)[:, None]
    outgoing = jnp.dot(
        slot_match.astype(jnp.bfloat16), p["sens"], preferred_element_type=jnp.float32
    ).astype(jnp.bfloat16)
    code = (p["offset"] + 1) * resp_local + p["resp"]
    codes = jnp.sum(jnp.where(slot_match, code[None, :], 0), axis=1)
    codes = codes.reshape(devices, capacity)
    target_out = codes // resp_local - 1
    resp_out = codes - codes // resp_local * resp_local
    normed_blocks = p["normed"].reshape(resp_local, devices, cols).transpose(1, 0, 2)
    meta = jnp.concatenate(
        [
            lane_pad(target_out.astype(jnp.float32), lanes),
            lane_pad(resp_out.astype(jnp.float32), lanes),
            lane_pad(jnp.broadcast_to(p["own_reward"][None, :], (devices, resp_local)), lanes),
            jnp.zeros((devices, 1, lanes), jnp.float32),
            jnp.pad(normed_blocks, ((0, 0), (0, 0), (0, lanes - cols))),
        ],
        axis=1,
    )
    extra = -meta.shape[1] % 8
    meta = jnp.pad(meta, ((0, 0), (0, extra), (0, 0)))
    meta_in, arrived = exchange(
        meta, outgoing.reshape(devices, capacity, width), devices, n_dev
    )
    targets = meta_in[:, 0, :capacity].astype(jnp.int32).reshape(devices * capacity)
    resp_in = meta_in[:, 1, :capacity].astype(jnp.int32)
    reward = meta_in[:, 2, :resp_local].reshape(responses)
    normed_in = meta_in[:, 4 : 4 + resp_local, :cols]
    reward_grad = reward_grads(p, reward).reshape(devices, resp_local)
    head_grad = jnp.sum(reward_grad[:, :, None] * normed_in, axis=(0, 1))
    resp_hot = resp_in[:, :, None] == jnp.arange(resp_local, dtype=jnp.int32)[None, None, :]
    scale = jnp.sum(jnp.where(resp_hot, reward_grad[:, None, :], 0.0), axis=2)
    total = devices * capacity
    owned = place_all(
        p["shard_rows"], arrived.reshape(total, width), targets, scale.reshape(total)
    )
    return owned, head_grad


def relay_local(*args):
    n_grp, n_dev = lax.axis_size("grp"), lax.axis_size("dev")
    p = prepare(*args)
    devices, resp_local, width = p["devices"], p["resp_local"], p["width"]
    hd = n_dev // 2
    local_n = devices // 2
    pieces = n_grp + 1
    cols = width // devices
    responses = devices * resp_local
    g, v = lax.axis_index("grp"), lax.axis_index("dev")
    half = v // hd
    me = g * n_dev + v
    owner, rank, live = p["owner"], p["rank"], p["live"]
    owner_g, owner_v = owner // n_dev, owner % n_dev
    owner_local = owner_g * hd + owner_v % hd
    near = owner_v // hd == half
    dev_ids = jnp.arange(devices, dtype=jnp.int32)
    dev_far = dev_ids % n_dev // hd != half
    over = jnp.where(dev_far, jnp.maximum(p["counts"] - FAR, 0), 0)
    over_base = jnp.sum(jnp.where(dev_ids[None, :] < dev_ids[:, None], over[None, :], 0), axis=1)
    j = jnp.sum(jnp.where(p["owner_hot"], over_base[None, :], 0), axis=1) + rank - FAR
    far_start = local_n * NEAR
    piece_start = far_start + local_n * FAR
    slots = piece_start + pieces * GROUP
    piece_slot = jnp.where(
        j < pieces * GROUP, piece_start + j % pieces * GROUP + j // pieces, -1
    )
    slot = jnp.where(
        near,
        owner_local * NEAR + rank,
        jnp.where(rank < FAR, far_start + owner_local * FAR + rank, piece_slot),
    )
    slot = jnp.where(live, slot, -1)
    slot_match = slot[None, :] == jnp.arange(slots, dtype=jnp.int32)[:, None]
    outgoing = jnp.dot(
        slot_match.astype(jnp.bfloat16), p["sens"], preferred_element_type=jnp.float32
    ).astype(jnp.bfloat16)
    code = (p["offset"] + 1) * responses + me * resp_local + p["resp"]
    shown = jnp.where(near | (rank < FAR), rank, -1)
    direct = jnp.where(live & (shown >= 0), owner * NEAR + shown, -1)
    direct_match = direct[None, :] == jnp.arange(devices * NEAR, dtype=jnp.int32)[:, None]
    codes = jnp.sum(jnp.where(direct_match, code[None, :], 0), axis=1).reshape(devices, NEAR)
    piece_match = slot_match[piece_start:]
    piece_code = jnp.sum(jnp.where(piece_match, code[None, :], 0), axis=1)
    piece_owner = jnp.sum(jnp.where(piece_match, owner_local[None, :], 0), axis=1)
    piece_target = piece_code // responses
    lane = jnp.arange(128, dtype=jnp.int32)[None, :]
    pmeta = jnp.zeros((pieces * GROUP, 128), jnp.int32)
    for i, col in enumerate(
        (
            (piece_code > 0).astype(jnp.int32),
            piece_owner // hd,
            piece_owner % hd,
            piece_code % responses,
            piece_target // 64,
            piece_target % 64,
        )
    ):
        pmeta = jnp.where(lane == i, col[:, None], pmeta)
    pmeta = pmeta.astype(jnp.float32).reshape(pieces, GROUP, 128)
    normed_blocks = p["normed"].reshape(resp_local, devices, cols).transpose(1, 0, 2)
    fm = jnp.concatenate(
        [
            lane_pad(jnp.broadcast_to(p["own_reward"][None, :], (devices, resp_local)), 128),
            lane_pad(codes.astype(jnp.float32), 128),
            lane_pad(jnp.broadcast_to(over.astype(jnp.float32)[None, :], (devices, devices)), 128),
            jnp.zeros((devices, 1, 128), jnp.float32),
            jnp.pad(normed_blocks, ((0, 0), (0, 4 - resp_local), (0, 128 - cols))),
        ],
        axis=1,
    )
    fm_in, rows_in, fmeta_in = relay_exchange(
        fm, outgoing.reshape(slots // GROUP, GROUP, width), pmeta, n_grp, n_dev
    )

    reward = fm_in[:, 0, :resp_local].reshape(responses)
    reward_grad = reward_grads(p, reward)
    normed_in = fm_in[:, 4 : 4 + resp_local, :cols]
    head_grad = jnp.sum(
        reward_grad.reshape(devices, resp_local)[:, :, None] * normed_in, axis=(0, 1)
    )
    all_codes = fm_in[:, 1, :NEAR].astype(jnp.int32).reshape(n_grp, 2, hd, NEAR)
    near_codes = jnp.where(half == 0, all_codes[:, 0], all_codes[:, 1])
    far_codes = jnp.where(half == 0, all_codes[:, 1], all_codes[:, 0])[..., :FAR]
    fmeta = fmeta_in.astype(jnp.int32)
    fwd_codes = (fmeta[..., 4] * 64 + fmeta[..., 5]) * responses + fmeta[..., 3]
    in_codes = jnp.concatenate(
        [near_codes.reshape(-1), far_codes.reshape(-1), fwd_codes.reshape(-1)]
    )
    targets = in_codes // responses - 1
    resp_in = in_codes % responses
    resp_hot = resp_in[:, None] == jnp.arange(responses, dtype=jnp.int32)[None, :]
    scale = jnp.sum(jnp.where(resp_hot, reward_grad[None, :], 0.0), axis=1)

    over_all = fm_in[:, 2, :devices].astype(jnp.int32)
    same = dev_ids[:, None] < dev_ids[None, :]
    base_all = jnp.sum(jnp.where(same[None], over_all[:, :, None], 0), axis=1)
    src_g, src_u = dev_ids // n_dev, dev_ids % hd
    here_g = jnp.arange(local_n, dtype=jnp.int32) // hd
    here_u = jnp.arange(local_n, dtype=jnp.int32) % hd
    load = jnp.zeros((local_n, devices), jnp.int32)
    for q in range(pieces):
        cnt = (base_all + over_all - q + pieces - 1) // pieces - (
            base_all - q + pieces - 1
        ) // pieces
        if q < n_grp:
            lands = ((src_g[None, :] + q) % n_grp == here_g[:, None]) & (
                src_u[None, :] == here_u[:, None]
            )
        else:
            lands = (src_g[None, :] == here_g[:, None]) & (
                (src_u[None, :] + hd // 2) % hd == here_u[:, None]
            )
        load = load + jnp.sum(jnp.where(lands[:, :, None], cnt[None], 0), axis=1)
    fits = (jnp.max(load) <= FWD) & (jnp.max(jnp.sum(over_all, axis=1)) <= pieces * GROUP)

    total = rows_in.shape[0] * GROUP
    rows = rows_in.reshape(total, width)

    def relayed(operands):
        rows, targets, scale = operands
        return place_rows(p["shard_rows"], rows, targets, scale)

    def resend(operands):
        return plain_finish(p, n_dev)[0]

    owned = lax.cond(fits, relayed, resend, (rows, targets, scale))
    return owned, head_grad


def place_rows(shard_rows, rows, targets, scale):
    total, width = rows.shape
    blocks, window = 3, 256
    block_rows = shard_rows // blocks
    first_row = jnp.arange(blocks, dtype=jnp.int32) * block_rows
    in_block = (targets[:, None] >= first_row[None, :]) & (
        targets[:, None] < first_row[None, :] + block_rows
    )
    block_hot = in_block.astype(jnp.bfloat16)
    pos = jnp.arange(total, dtype=jnp.int32)
    ahead = (pos[:, None] > pos[None, :]).astype(jnp.bfloat16)
    rank_in = jnp.dot(ahead, block_hot, preferred_element_type=jnp.float32).astype(jnp.int32)
    slot_base = jnp.arange(blocks, dtype=jnp.int32) * window
    packed_slot = jnp.sum(jnp.where(in_block, rank_in + slot_base[None, :] + 1, 0), axis=1) - 1
    fits = jnp.max(jnp.sum(in_block.astype(jnp.int32), axis=0)) <= window

    def packed_place(operands):
        rows, targets, scale = operands
        pack = packed_slot[None, :] == jnp.arange(blocks * window, dtype=jnp.int32)[:, None]
        packed_scale = jnp.sum(jnp.where(pack, scale[None, :], 0.0), axis=1)
        packed_target = jnp.sum(jnp.where(pack, targets[None, :] + 1, 0), axis=1) - 1
        packed = jnp.dot(pack.astype(jnp.bfloat16), rows, preferred_element_type=jnp.float32)
        packed = (packed_scale[:, None] * packed).astype(jnp.bfloat16)
        row_of = first_row[:, None] + jnp.arange(block_rows, dtype=jnp.int32)[None, :]
        placing = packed_target.reshape(blocks, 1, window) == row_of[:, :, None]
        owned = lax.dot_general(
            placing.astype(jnp.bfloat16),
            packed.reshape(blocks, window, width),
            (((2,), (1,)), ((0,), (0,))),
            preferred_element_type=jnp.float32,
        )
        return owned.astype(jnp.bfloat16).reshape(shard_rows, width)

    return lax.cond(
        fits, packed_place, lambda o: place_all(shard_rows, *o), (rows, targets, scale)
    )


def solution(mesh):
    placed = (
        P(("grp", "dev"), None),
        P(("grp", "dev"), None, None),
        P(("grp", "dev"), None),
        P(("grp", "dev")),
        P(),
        P(),
        P(),
        P(),
        P(),
    )
    return jax.shard_map(
        local,
        mesh=mesh,
        in_specs=placed,
        out_specs=(P(("grp", "dev"), None), P(("grp", "dev"))),
        check_vma=False,
    )
```

```python
import functools

import jax
import jax.numpy as jnp
from jax import lax
from jax.experimental import pallas as pl
from jax.experimental.pallas import tpu as pltpu
from jax.sharding import PartitionSpec as P

VOCAB = 128256
MESH = pl.DeviceIdType.MESH


def exchange_kernel(n, n_dev, meta_ref, rows_ref, meta_out, rows_out, send_sem, recv_sem, own_sem):
    me = lax.axis_index("grp") * n_dev + lax.axis_index("dev")

    def coord(t):
        return (t // n_dev, lax.rem(t, n_dev))

    barrier = pltpu.get_barrier_semaphore()

    def greet(k, c):
        t = lax.rem(me + k, n)
        pl.semaphore_signal(barrier, inc=1, device_id=coord(t), device_id_type=MESH)
        return c

    lax.fori_loop(1, n, greet, 0)
    own = [
        pltpu.make_async_copy(src.at[me], dst.at[me], own_sem.at[i])
        for i, (src, dst) in enumerate(((meta_ref, meta_out), (rows_ref, rows_out)))
    ]
    for c in own:
        c.start()
    pl.semaphore_wait(barrier, n - 1)

    def copies(src_block, dst_block, to):
        return [
            pltpu.make_async_remote_copy(
                src_ref=src.at[src_block],
                dst_ref=dst.at[dst_block],
                send_sem=send_sem.at[i, src_block],
                recv_sem=recv_sem.at[i, dst_block],
                device_id=coord(to),
                device_id_type=MESH,
            )
            for i, (src, dst) in enumerate(((meta_ref, meta_out), (rows_ref, rows_out)))
        ]

    def send(k, c):
        t = lax.rem(me + k, n)
        for cp in copies(t, me, t):
            cp.start()
        return c

    lax.fori_loop(1, n, send, 0)

    def finish(k, c):
        t = lax.rem(me + k, n)
        for cp in copies(t, me, t):
            cp.wait_send()
        s = lax.rem(me + n - k, n)
        for cp in copies(s, s, s):
            cp.wait_recv()
        return c

    lax.fori_loop(1, n, finish, 0)
    for c in own:
        c.wait()


def exchange(meta, rows, n, n_dev):
    anyspec = pl.BlockSpec(memory_space=pl.ANY)
    return pl.pallas_call(
        functools.partial(exchange_kernel, n, n_dev),
        out_shape=(
            jax.ShapeDtypeStruct(meta.shape, meta.dtype),
            jax.ShapeDtypeStruct(rows.shape, rows.dtype),
        ),
        in_specs=[anyspec, anyspec],
        out_specs=(anyspec, anyspec),
        scratch_shapes=[
            pltpu.SemaphoreType.DMA((2, n)),
            pltpu.SemaphoreType.DMA((2, n)),
            pltpu.SemaphoreType.DMA((2,)),
        ],
        compiler_params=pltpu.CompilerParams(collective_id=1, has_side_effects=True),
    )(meta, rows)


GROUP = 8
NEAR = 32
FAR = 16
FWD = 8


def relay_kernel(n_grp, n_dev, fm_ref, slots_ref, pmeta_ref, fm_out, rows_out, fmeta_out,
                 pin, pmeta_in, fwd, fwd_meta, fm_sems, near_sems, far_sems, piece_sems,
                 pm_sems, fwd_sems, fwdm_sems, own_sems):
    g = lax.axis_index("grp")
    v = lax.axis_index("dev")
    hd = n_dev // 2
    local_n = n_grp * hd
    half = v // hd
    u = lax.rem(v, hd)
    me = g * n_dev + v
    me_local = g * hd + u
    n = n_grp * n_dev
    pieces = n_grp + 1
    near_g, far_g = NEAR // GROUP, FAR // GROUP
    far_base = local_n * near_g
    piece_base = far_base + local_n * far_g
    fwd_base = piece_base
    other = 1 - half

    def coord(t):
        return (t // n_dev, lax.rem(t, n_dev))

    barrier = pltpu.get_barrier_semaphore()

    def greet(k, c):
        pl.semaphore_signal(
            barrier, inc=1, device_id=coord(lax.rem(me + k, n)), device_id_type=MESH
        )
        return c

    lax.fori_loop(1, n, greet, 0)

    def local_copy(src, dst, i):
        return pltpu.make_async_copy(src, dst, own_sems.at[i])

    own = [
        local_copy(fm_ref.at[me], fm_out.at[me], 0),
        local_copy(
            slots_ref.at[pl.ds(me_local * near_g, near_g)],
            rows_out.at[pl.ds(me_local * near_g, near_g)],
            1,
        ),
    ]
    for cp in own:
        cp.start()
    pl.semaphore_wait(barrier, n - 1)

    def remote(src, dst, send_sem, recv_sem, to):
        return pltpu.make_async_remote_copy(
            src_ref=src,
            dst_ref=dst,
            send_sem=send_sem,
            recv_sem=recv_sem,
            device_id=to,
            device_id_type=MESH,
        )

    def piece_target(q):
        if q < n_grp:
            return (lax.rem(g + q, n_grp), other * hd + u)
        return (g, other * hd + lax.rem(u + hd // 2, hd))

    piece_copies = []
    for q in range(pieces):
        to = piece_target(q)
        piece_copies.append(
            remote(slots_ref.at[piece_base + q], pin.at[q],
                   piece_sems.at[0, q], piece_sems.at[1, q], to)
        )
        piece_copies.append(
            remote(pmeta_ref.at[q], pmeta_in.at[q], pm_sems.at[0, q], pm_sems.at[1, q], to)
        )
    for cp in piece_copies:
        cp.start()

    def fm_copy(src, dst, k):
        return remote(fm_ref.at[src], fm_out.at[dst], fm_sems.at[0, k], fm_sems.at[1, k],
                      coord(src))

    def split(k):
        a = k // hd
        b = lax.rem(k, hd)
        return a, b

    def near_copy(k):
        a, b = split(k)
        tg, tu = lax.rem(g + a, n_grp), lax.rem(u + b, hd)
        t = tg * hd + tu
        return remote(
            slots_ref.at[pl.ds(t * near_g, near_g)],
            rows_out.at[pl.ds(me_local * near_g, near_g)],
            near_sems.at[0, k],
            near_sems.at[1, k],
            (tg, half * hd + tu),
        )

    def far_copy(k):
        a, b = split(k)
        tg, tu = lax.rem(g + a, n_grp), lax.rem(u + b, hd)
        t = tg * hd + tu
        return remote(
            slots_ref.at[pl.ds(far_base + t * far_g, far_g)],
            rows_out.at[pl.ds(far_base + me_local * far_g, far_g)],
            far_sems.at[0, k],
            far_sems.at[1, k],
            (tg, other * hd + tu),
        )

    def send_fm(k, c):
        fm_copy(lax.rem(me + k, n), me, k).start()
        return c

    lax.fori_loop(1, n, send_fm, 0)

    def send_far(k, c):
        far_copy(k).start()
        return c

    def send_near(k, c):
        near_copy(k).start()
        return c

    far_copy(0).start()

    def send_both(k, c):
        far_copy(k).start()
        near_copy(k).start()
        return c

    lax.fori_loop(1, 16, send_both, 0)

    for cp in piece_copies:
        cp.wait_recv()
    count = pieces * GROUP
    marks = pmeta_in[...].reshape(count, 128)
    used = marks[:, 0:1] > 0.0
    dst = (marks[:, 1:2] * hd + marks[:, 2:3]).astype(jnp.int32)
    lane = lax.broadcasted_iota(jnp.int32, (count, 128), 1)
    hot = jnp.where((lane == dst) & used, 1.0, 0.0)
    row_i = lax.broadcasted_iota(jnp.int32, (count, count), 0)
    col_i = lax.broadcasted_iota(jnp.int32, (count, count), 1)
    earlier = jnp.where(row_i > col_i, 1.0, 0.0)
    before = jnp.dot(earlier, hot, preferred_element_type=jnp.float32)
    rank = jnp.sum(before * hot, axis=1, keepdims=True).astype(jnp.int32)
    slot = jnp.where(used & (rank < FWD), dst * FWD + rank, -1)
    place = jnp.where(lane == slot, 1.0, 0.0)
    contract = (((0,), (0,)), ((), ()))
    width = pin.shape[2]
    chunk = 512

    def gather(c, carry):
        cols = pl.ds(pl.multiple_of(c * chunk, chunk), chunk)
        rows = pin[:, :, cols].astype(jnp.float32).reshape(count, chunk)
        out = lax.dot_general(place, rows, contract, preferred_element_type=jnp.float32)
        fwd[:, :, cols] = out.reshape(local_n, FWD, chunk).astype(jnp.bfloat16)
        return carry

    lax.fori_loop(0, width // chunk, gather, 0)
    fwd_meta[...] = lax.dot_general(
        place, marks, contract, preferred_element_type=jnp.float32
    ).reshape(local_n, FWD, 128)

    def fwd_copies(k):
        a, b = split(k)
        tg, tu = lax.rem(g + a, n_grp), lax.rem(u + b, hd)
        t = tg * hd + tu
        to = (tg, half * hd + tu)
        return [
            remote(fwd.at[t], rows_out.at[fwd_base + me_local],
                   fwd_sems.at[0, k], fwd_sems.at[1, k], to),
            remote(fwd_meta.at[t], fmeta_out.at[me_local],
                   fwdm_sems.at[0, k], fwdm_sems.at[1, k], to),
        ]

    own_fwd = [
        local_copy(fwd.at[me_local], rows_out.at[fwd_base + me_local], 2),
        local_copy(fwd_meta.at[me_local], fmeta_out.at[me_local], 3),
    ]
    for cp in own_fwd:
        cp.start()

    def send_fwd(k, c):
        for cp in fwd_copies(k):
            cp.start()
        return c

    lax.fori_loop(1, local_n, send_fwd, 0)
    lax.fori_loop(16, local_n, send_both, 0)

    for cp in piece_copies:
        cp.wait_send()

    def finish_far(k, c):
        cp = far_copy(k)
        cp.wait_send()
        cp.wait_recv()
        return c

    def finish_near(k, c):
        for cp in [near_copy(k)] + fwd_copies(k):
            cp.wait_send()
            cp.wait_recv()
        return c

    def finish_fm(k, c):
        cp = fm_copy(lax.rem(me + k, n), me, k)
        cp.wait_send()
        cp.wait_recv()
        return c

    lax.fori_loop(1, n, finish_fm, 0)
    lax.fori_loop(0, local_n, finish_far, 0)
    lax.fori_loop(1, local_n, finish_near, 0)
    for cp in own + own_fwd:
        cp.wait()


def relay_exchange(fm, slots, pmeta, n_grp, n_dev):
    n = n_grp * n_dev
    local_n = n // 2
    width = slots.shape[2]
    pieces = n_grp + 1
    groups = local_n * (NEAR + FAR + FWD) // GROUP
    anyspec = pl.BlockSpec(memory_space=pl.ANY)
    sem = pltpu.SemaphoreType.DMA
    return pl.pallas_call(
        functools.partial(relay_kernel, n_grp, n_dev),
        out_shape=(
            jax.ShapeDtypeStruct(fm.shape, fm.dtype),
            jax.ShapeDtypeStruct((groups, GROUP, width), slots.dtype),
            jax.ShapeDtypeStruct((local_n, FWD, 128), jnp.float32),
        ),
        in_specs=[anyspec, anyspec, anyspec],
        out_specs=(anyspec, anyspec, anyspec),
        scratch_shapes=[
            pltpu.VMEM((pieces, GROUP, width), slots.dtype),
            pltpu.VMEM((pieces, GROUP, 128), jnp.float32),
            pltpu.VMEM((local_n, FWD, width), slots.dtype),
            pltpu.VMEM((local_n, FWD, 128), jnp.float32),
            sem((2, n)),
            sem((2, local_n)),
            sem((2, local_n)),
            sem((2, pieces)),
            sem((2, pieces)),
            sem((2, local_n)),
            sem((2, local_n)),
            sem((4,)),
        ],
        compiler_params=pltpu.CompilerParams(collective_id=0, has_side_effects=True),
    )(fm, slots, pmeta)


def local(token_ids, sensitivity, last_hidden, lengths, norm_gain, reward_head,
          chosen_index, rejected_index, shard_owner):
    args = (token_ids, sensitivity, last_hidden, lengths, norm_gain, reward_head,
            chosen_index, rejected_index, shard_owner)
    resp_local, block_len = token_ids.shape
    devices = shard_owner.shape[0]
    n_grp, n_dev = lax.axis_size("grp"), lax.axis_size("dev")
    capacity = max(2, (2 * resp_local * block_len + devices - 1) // devices)
    if (capacity == NEAR and n_dev % 4 == 0 and devices * resp_local <= 128
            and resp_local <= 4 and devices // 2 * FWD <= 128
            and VOCAB // devices < 64 * 250):
        return relay_local(*args)
    prep = prepare(*args)
    return plain_finish(prep, n_dev)


def prepare(token_ids, sensitivity, last_hidden, lengths, norm_gain, reward_head,
            chosen_index, rejected_index, shard_owner):
    resp_local, block_len = token_ids.shape
    width = sensitivity.shape[2]
    tok_local = resp_local * block_len
    devices = shard_owner.shape[0]
    shard_rows = VOCAB // devices
    capacity = max(2, (2 * tok_local + devices - 1) // devices)
    hidden = last_hidden.astype(jnp.float32)
    normed = (
        hidden / jnp.sqrt(jnp.mean(hidden * hidden, axis=-1, keepdims=True) + 1e-05) * norm_gain
    )
    own_reward = jnp.sum(normed * reward_head, axis=-1)

    positions = jnp.arange(block_len, dtype=jnp.int32)
    live = (positions[None, :] < lengths[:, None]).reshape(tok_local)
    ids = token_ids.reshape(tok_local)
    shard_of = ids // shard_rows
    offset = ids - shard_of * shard_rows
    shard_hot = shard_of[:, None] == jnp.arange(devices, dtype=jnp.int32)[None, :]
    owner = jnp.sum(jnp.where(shard_hot, shard_owner[None, :], 0), axis=1)
    owner_hot = (owner[:, None] == jnp.arange(devices, dtype=jnp.int32)[None, :]) & live[:, None]
    live_hot = owner_hot.astype(jnp.bfloat16)
    token_pos = jnp.arange(tok_local, dtype=jnp.int32)
    earlier = (token_pos[:, None] > token_pos[None, :]).astype(jnp.bfloat16)
    before = jnp.dot(earlier, live_hot, preferred_element_type=jnp.float32)
    rank = jnp.sum(before * live_hot.astype(jnp.float32), axis=1).astype(jnp.int32)
    counts = jnp.sum(owner_hot.astype(jnp.int32), axis=0)
    return dict(
        sens=sensitivity.reshape(tok_local, width), normed=normed, own_reward=own_reward,
        live=live, offset=offset, owner=owner, rank=rank, counts=counts,
        owner_hot=owner_hot, resp=token_pos // block_len, capacity=capacity,
        chosen_index=chosen_index, rejected_index=rejected_index, devices=devices,
        shard_rows=shard_rows, resp_local=resp_local, width=width, tok_local=tok_local,
    )


def lane_pad(a, lanes):
    return jnp.pad(a, ((0, 0), (0, lanes - a.shape[1])))[:, None, :]


def reward_grads(p, reward):
    responses = p["devices"] * p["resp_local"]
    all_resp = jnp.arange(responses, dtype=jnp.int32)
    sign_table = (p["chosen_index"][:, None] == all_resp[None, :]).astype(jnp.float32) - (
        p["rejected_index"][:, None] == all_resp[None, :]
    ).astype(jnp.float32)
    margin = jnp.sum(sign_table * reward[None, :], axis=1)
    push = -jax.nn.sigmoid(-margin)
    return jnp.sum(sign_table * push[:, None], axis=0)


def place_all(shard_rows, rows, targets, scale):
    scaled = (scale[:, None] * rows).astype(jnp.bfloat16)
    placing = (targets[None, :] == jnp.arange(shard_rows, dtype=jnp.int32)[:, None]).astype(
        jnp.bfloat16
    )
    return jnp.dot(placing, scaled, preferred_element_type=jnp.float32).astype(jnp.bfloat16)


def plain_finish(p, n_dev):
    devices, capacity, resp_local = p["devices"], p["capacity"], p["resp_local"]
    width = p["width"]
    cols = width // devices
    responses = devices * resp_local
    lanes = -(-max(cols, capacity, resp_local) // 128) * 128
    slot = jnp.where(p["live"], p["owner"] * capacity + p["rank"], -1)
    slot_match = slot[None, :] == jnp.arange(devices * capacity, dtype=jnp.int32)[:, None]
    outgoing = jnp.dot(
        slot_match.astype(jnp.bfloat16), p["sens"], preferred_element_type=jnp.float32
    ).astype(jnp.bfloat16)
    code = (p["offset"] + 1) * resp_local + p["resp"]
    codes = jnp.sum(jnp.where(slot_match, code[None, :], 0), axis=1)
    codes = codes.reshape(devices, capacity)
    target_out = codes // resp_local - 1
    resp_out = codes - codes // resp_local * resp_local
    normed_blocks = p["normed"].reshape(resp_local, devices, cols).transpose(1, 0, 2)
    meta = jnp.concatenate(
        [
            lane_pad(target_out.astype(jnp.float32), lanes),
            lane_pad(resp_out.astype(jnp.float32), lanes),
            lane_pad(jnp.broadcast_to(p["own_reward"][None, :], (devices, resp_local)), lanes),
            jnp.zeros((devices, 1, lanes), jnp.float32),
            jnp.pad(normed_blocks, ((0, 0), (0, 0), (0, lanes - cols))),
        ],
        axis=1,
    )
    extra = -meta.shape[1] % 8
    meta = jnp.pad(meta, ((0, 0), (0, extra), (0, 0)))
    meta_in, arrived = exchange(
        meta, outgoing.reshape(devices, capacity, width), devices, n_dev
    )
    targets = meta_in[:, 0, :capacity].astype(jnp.int32).reshape(devices * capacity)
    resp_in = meta_in[:, 1, :capacity].astype(jnp.int32)
    reward = meta_in[:, 2, :resp_local].reshape(responses)
    normed_in = meta_in[:, 4 : 4 + resp_local, :cols]
    reward_grad = reward_grads(p, reward).reshape(devices, resp_local)
    head_grad = jnp.sum(reward_grad[:, :, None] * normed_in, axis=(0, 1))
    resp_hot = resp_in[:, :, None] == jnp.arange(resp_local, dtype=jnp.int32)[None, None, :]
    scale = jnp.sum(jnp.where(resp_hot, reward_grad[:, None, :], 0.0), axis=2)
    total = devices * capacity
    owned = place_all(
        p["shard_rows"], arrived.reshape(total, width), targets, scale.reshape(total)
    )
    return owned, head_grad


def relay_local(*args):
    n_grp, n_dev = lax.axis_size("grp"), lax.axis_size("dev")
    p = prepare(*args)
    devices, resp_local, width = p["devices"], p["resp_local"], p["width"]
    hd = n_dev // 2
    local_n = devices // 2
    pieces = n_grp + 1
    cols = width // devices
    responses = devices * resp_local
    g, v = lax.axis_index("grp"), lax.axis_index("dev")
    half = v // hd
    me = g * n_dev + v
    owner, rank, live = p["owner"], p["rank"], p["live"]
    owner_g, owner_v = owner // n_dev, owner % n_dev
    owner_local = owner_g * hd + owner_v % hd
    near = owner_v // hd == half
    dev_ids = jnp.arange(devices, dtype=jnp.int32)
    dev_far = dev_ids % n_dev // hd != half
    over = jnp.where(dev_far, jnp.maximum(p["counts"] - FAR, 0), 0)
    over_base = jnp.sum(jnp.where(dev_ids[None, :] < dev_ids[:, None], over[None, :], 0), axis=1)
    j = jnp.sum(jnp.where(p["owner_hot"], over_base[None, :], 0), axis=1) + rank - FAR
    far_start = local_n * NEAR
    piece_start = far_start + local_n * FAR
    slots = piece_start + pieces * GROUP
    piece_slot = jnp.where(
        j < pieces * GROUP, piece_start + j % pieces * GROUP + j // pieces, -1
    )
    slot = jnp.where(
        near,
        owner_local * NEAR + rank,
        jnp.where(rank < FAR, far_start + owner_local * FAR + rank, piece_slot),
    )
    slot = jnp.where(live, slot, -1)
    slot_match = slot[None, :] == jnp.arange(slots, dtype=jnp.int32)[:, None]
    outgoing = jnp.dot(
        slot_match.astype(jnp.bfloat16), p["sens"], preferred_element_type=jnp.float32
    ).astype(jnp.bfloat16)
    code = (p["offset"] + 1) * responses + me * resp_local + p["resp"]
    shown = jnp.where(near | (rank < FAR), rank, -1)
    direct = jnp.where(live & (shown >= 0), owner * NEAR + shown, -1)
    direct_match = direct[None, :] == jnp.arange(devices * NEAR, dtype=jnp.int32)[:, None]
    codes = jnp.sum(jnp.where(direct_match, code[None, :], 0), axis=1).reshape(devices, NEAR)
    piece_match = slot_match[piece_start:]
    piece_code = jnp.sum(jnp.where(piece_match, code[None, :], 0), axis=1)
    piece_owner = jnp.sum(jnp.where(piece_match, owner_local[None, :], 0), axis=1)
    piece_target = piece_code // responses
    lane = jnp.arange(128, dtype=jnp.int32)[None, :]
    pmeta = jnp.zeros((pieces * GROUP, 128), jnp.int32)
    for i, col in enumerate(
        (
            (piece_code > 0).astype(jnp.int32),
            piece_owner // hd,
            piece_owner % hd,
            piece_code % responses,
            piece_target // 64,
            piece_target % 64,
        )
    ):
        pmeta = jnp.where(lane == i, col[:, None], pmeta)
    pmeta = pmeta.astype(jnp.float32).reshape(pieces, GROUP, 128)
    normed_blocks = p["normed"].reshape(resp_local, devices, cols).transpose(1, 0, 2)
    fm = jnp.concatenate(
        [
            lane_pad(jnp.broadcast_to(p["own_reward"][None, :], (devices, resp_local)), 128),
            lane_pad(codes.astype(jnp.float32), 128),
            lane_pad(jnp.broadcast_to(over.astype(jnp.float32)[None, :], (devices, devices)), 128),
            jnp.zeros((devices, 1, 128), jnp.float32),
            jnp.pad(normed_blocks, ((0, 0), (0, 4 - resp_local), (0, 128 - cols))),
        ],
        axis=1,
    )
    fm_in, rows_in, fmeta_in = relay_exchange(
        fm, outgoing.reshape(slots // GROUP, GROUP, width), pmeta, n_grp, n_dev
    )

    reward = fm_in[:, 0, :resp_local].reshape(responses)
    reward_grad = reward_grads(p, reward)
    normed_in = fm_in[:, 4 : 4 + resp_local, :cols]
    head_grad = jnp.sum(
        reward_grad.reshape(devices, resp_local)[:, :, None] * normed_in, axis=(0, 1)
    )
    all_codes = fm_in[:, 1, :NEAR].astype(jnp.int32).reshape(n_grp, 2, hd, NEAR)
    near_codes = jnp.where(half == 0, all_codes[:, 0], all_codes[:, 1])
    far_codes = jnp.where(half == 0, all_codes[:, 1], all_codes[:, 0])[..., :FAR]
    fmeta = fmeta_in.astype(jnp.int32)
    fwd_codes = (fmeta[..., 4] * 64 + fmeta[..., 5]) * responses + fmeta[..., 3]
    in_codes = jnp.concatenate(
        [near_codes.reshape(-1), far_codes.reshape(-1), fwd_codes.reshape(-1)]
    )
    targets = in_codes // responses - 1
    resp_in = in_codes % responses
    resp_hot = resp_in[:, None] == jnp.arange(responses, dtype=jnp.int32)[None, :]
    scale = jnp.sum(jnp.where(resp_hot, reward_grad[None, :], 0.0), axis=1)

    over_all = fm_in[:, 2, :devices].astype(jnp.int32)
    same = dev_ids[:, None] < dev_ids[None, :]
    base_all = jnp.sum(jnp.where(same[None], over_all[:, :, None], 0), axis=1)
    src_g, src_u = dev_ids // n_dev, dev_ids % hd
    here_g = jnp.arange(local_n, dtype=jnp.int32) // hd
    here_u = jnp.arange(local_n, dtype=jnp.int32) % hd
    load = jnp.zeros((local_n, devices), jnp.int32)
    for q in range(pieces):
        cnt = (base_all + over_all - q + pieces - 1) // pieces - (
            base_all - q + pieces - 1
        ) // pieces
        if q < n_grp:
            lands = ((src_g[None, :] + q) % n_grp == here_g[:, None]) & (
                src_u[None, :] == here_u[:, None]
            )
        else:
            lands = (src_g[None, :] == here_g[:, None]) & (
                (src_u[None, :] + hd // 2) % hd == here_u[:, None]
            )
        load = load + jnp.sum(jnp.where(lands[:, :, None], cnt[None], 0), axis=1)
    fits = (jnp.max(load) <= FWD) & (jnp.max(jnp.sum(over_all, axis=1)) <= pieces * GROUP)

    total = rows_in.shape[0] * GROUP
    rows = rows_in.reshape(total, width)

    def relayed(operands):
        rows, targets, scale = operands
        return place_rows(p["shard_rows"], rows, targets, scale)

    def resend(operands):
        return plain_finish(p, n_dev)[0]

    owned = lax.cond(fits, relayed, resend, (rows, targets, scale))
    return owned, head_grad


MAIN = 640
CHUNK = 512
BLOCK_ROWS = 512


def place_kernel(count_ref, starts_ref, pos_ref, target_ref, scale_ref, rows_ref, out_ref,
                 rows_v, sorted_v, pick, onehot, acc, outbuf, in_sems, out_sems):
    total, width = rows_ref.shape
    shard_rows = out_ref.shape[0]
    chunks = width // CHUNK
    blocks = -(-shard_rows // BLOCK_ROWS)

    def fetch(c):
        return pltpu.make_async_copy(
            rows_ref.at[:, pl.ds(c * CHUNK, CHUNK)], rows_v.at[c], in_sems.at[c]
        )

    for c in range(chunks):
        fetch(c).start()
    rows_id = lax.broadcasted_iota(jnp.int32, (MAIN, total), 0)
    pick[...] = jnp.where(rows_id == pos_ref[0:1, :], 1.0, 0.0).astype(jnp.bfloat16)
    count = count_ref[0]
    used = lax.max(lax.div(count + 127, 128), MAIN // 128)

    for c in range(chunks):
        fetch(c).wait()
        got = jnp.dot(pick[...], rows_v[c], preferred_element_type=jnp.float32)
        sorted_v[pl.ds(0, MAIN), pl.ds(c * CHUNK, CHUNK)] = (
            scale_ref[pl.ds(0, MAIN), :] * got
        ).astype(jnp.bfloat16)

    def extra(m, carry):
        base = pl.multiple_of(m * 128, 128)
        ids = lax.broadcasted_iota(jnp.int32, (128, total), 0) + base
        sel = jnp.where(ids == pos_ref[0:1, :], 1.0, 0.0).astype(jnp.bfloat16)
        for c in range(chunks):
            got = jnp.dot(sel, rows_v[c], preferred_element_type=jnp.float32)
            sorted_v[pl.ds(base, 128), pl.ds(c * CHUNK, CHUNK)] = (
                scale_ref[pl.ds(base, 128), :] * got
            ).astype(jnp.bfloat16)
        return carry

    lax.fori_loop(MAIN // 128, used, extra, 0)
    sorted_v[pl.ds(pl.multiple_of(used * 128, 128), 128), :] = jnp.zeros(
        (128, width), jnp.bfloat16
    )

    def put(b):
        size = min(BLOCK_ROWS, shard_rows - b * BLOCK_ROWS)
        return pltpu.make_async_copy(
            outbuf.at[b % 2, pl.ds(0, size)],
            out_ref.at[pl.ds(b * BLOCK_ROWS, size)],
            out_sems.at[b % 2],
        )

    for b in range(blocks):
        size = min(BLOCK_ROWS, shard_rows - b * BLOCK_ROWS)
        size16 = -(-size // 16) * 16
        first, last = starts_ref[b], starts_ref[b + 1]
        low = lax.div(first, 128) * 128
        windows = lax.div(last - low + 255, 256)
        if b >= 2:
            put(b - 2).wait()
        row_id = lax.broadcasted_iota(jnp.int32, (size16, 256), 0) + b * BLOCK_ROWS

        def window(w):
            at = pl.multiple_of(low + w * 256, 128)
            return at, jnp.where(
                row_id == target_ref[0:1, pl.ds(at, 256)], 1.0, 0.0
            ).astype(jnp.bfloat16)

        @pl.when(windows <= 1)
        def _():
            at, hot = window(0)
            onehot[pl.ds(0, size16), :] = hot

            def col(c, carry):
                cols = pl.ds(pl.multiple_of(c * CHUNK, CHUNK), CHUNK)
                outbuf[b % 2, pl.ds(0, size16), cols] = jnp.dot(
                    onehot[pl.ds(0, size16), :],
                    sorted_v[pl.ds(at, 256), cols],
                    preferred_element_type=jnp.float32,
                ).astype(jnp.bfloat16)
                return carry

            lax.fori_loop(0, chunks, col, 0)

        @pl.when(windows > 1)
        def _():
            def col(c, carry):
                cols = pl.ds(pl.multiple_of(c * CHUNK, CHUNK), CHUNK)
                acc[...] = jnp.zeros_like(acc)

                def add(w, carry):
                    at, hot = window(w)
                    acc[pl.ds(0, size16), :] += jnp.dot(
                        hot, sorted_v[pl.ds(at, 256), cols],
                        preferred_element_type=jnp.float32,
                    )
                    return carry

                lax.fori_loop(0, windows, add, 0)
                outbuf[b % 2, pl.ds(0, size16), cols] = acc[pl.ds(0, size16), :].astype(
                    jnp.bfloat16
                )
                return carry

            lax.fori_loop(0, chunks, col, 0)

        put(b).start()
    for b in range(max(0, blocks - 2), blocks):
        put(b).wait()


def place_rows(shard_rows, rows, targets, scale):
    total, width = rows.shape
    cap = 1280
    chunks = width // CHUNK
    blocks = -(-shard_rows // BLOCK_ROWS)
    index = jnp.arange(total, dtype=jnp.int32)
    live = targets >= 0
    key = jnp.where(live, targets * 2048 + index, 1 << 30)
    pos = jnp.sum((key[:, None] < key[None, :]).astype(jnp.int32), axis=0)
    pos = jnp.where(live, pos, -1)
    place = jnp.arange(cap, dtype=jnp.int32)
    hot = pos[:, None] == place[None, :]
    sorted_target = jnp.sum(jnp.where(hot, targets[:, None] + 1, 0), axis=0) - 1
    sorted_scale = jnp.sum(
        jnp.where(pos[None, :] == place[:, None], scale[None, :], 0.0), axis=1
    )
    limit = jnp.arange(blocks + 1, dtype=jnp.int32) * BLOCK_ROWS
    starts = jnp.sum(
        (live[None, :] & (targets[None, :] < limit[:, None])).astype(jnp.int32), axis=1
    )
    smem = pl.BlockSpec(memory_space=pltpu.SMEM)
    vmem = pl.BlockSpec(memory_space=pltpu.VMEM)
    anyspec = pl.BlockSpec(memory_space=pl.ANY)
    return pl.pallas_call(
        place_kernel,
        out_shape=jax.ShapeDtypeStruct((shard_rows, width), rows.dtype),
        in_specs=[smem, smem, vmem, vmem, vmem, anyspec],
        out_specs=anyspec,
        scratch_shapes=[
            pltpu.VMEM((chunks, total, CHUNK), jnp.bfloat16),
            pltpu.VMEM((cap, width), jnp.bfloat16),
            pltpu.VMEM((MAIN, total), jnp.bfloat16),
            pltpu.VMEM((BLOCK_ROWS, 256), jnp.bfloat16),
            pltpu.VMEM((BLOCK_ROWS, CHUNK), jnp.float32),
            pltpu.VMEM((2, BLOCK_ROWS, width), jnp.bfloat16),
            pltpu.SemaphoreType.DMA((chunks,)),
            pltpu.SemaphoreType.DMA((2,)),
        ],
        compiler_params=pltpu.CompilerParams(vmem_limit_bytes=60 * 1024 * 1024),
    )(starts[blocks:], starts, pos[None, :], sorted_target[None, :], sorted_scale[:, None], rows)


def solution(mesh):
    placed = (
        P(("grp", "dev"), None),
        P(("grp", "dev"), None, None),
        P(("grp", "dev"), None),
        P(("grp", "dev")),
        P(),
        P(),
        P(),
        P(),
        P(),
    )
    return jax.shard_map(
        local,
        mesh=mesh,
        in_specs=placed,
        out_specs=(P(("grp", "dev"), None), P(("grp", "dev"))),
        check_vma=False,
    )
```

```python
import functools

import jax
import jax.numpy as jnp
from jax import lax
from jax.experimental import pallas as pl
from jax.experimental.pallas import tpu as pltpu
from jax.sharding import PartitionSpec as P

VOCAB = 128256
MESH = pl.DeviceIdType.MESH


def exchange_kernel(n, n_dev, meta_ref, rows_ref, meta_out, rows_out, send_sem, recv_sem, own_sem):
    me = lax.axis_index("grp") * n_dev + lax.axis_index("dev")

    def coord(t):
        return (t // n_dev, lax.rem(t, n_dev))

    barrier = pltpu.get_barrier_semaphore()

    def greet(k, c):
        t = lax.rem(me + k, n)
        pl.semaphore_signal(barrier, inc=1, device_id=coord(t), device_id_type=MESH)
        return c

    lax.fori_loop(1, n, greet, 0)
    own = [
        pltpu.make_async_copy(src.at[me], dst.at[me], own_sem.at[i])
        for i, (src, dst) in enumerate(((meta_ref, meta_out), (rows_ref, rows_out)))
    ]
    for c in own:
        c.start()
    pl.semaphore_wait(barrier, n - 1)

    def copies(src_block, dst_block, to):
        return [
            pltpu.make_async_remote_copy(
                src_ref=src.at[src_block],
                dst_ref=dst.at[dst_block],
                send_sem=send_sem.at[i, src_block],
                recv_sem=recv_sem.at[i, dst_block],
                device_id=coord(to),
                device_id_type=MESH,
            )
            for i, (src, dst) in enumerate(((meta_ref, meta_out), (rows_ref, rows_out)))
        ]

    def send(k, c):
        t = lax.rem(me + k, n)
        for cp in copies(t, me, t):
            cp.start()
        return c

    lax.fori_loop(1, n, send, 0)

    def finish(k, c):
        t = lax.rem(me + k, n)
        for cp in copies(t, me, t):
            cp.wait_send()
        s = lax.rem(me + n - k, n)
        for cp in copies(s, s, s):
            cp.wait_recv()
        return c

    lax.fori_loop(1, n, finish, 0)
    for c in own:
        c.wait()


def exchange(meta, rows, n, n_dev):
    anyspec = pl.BlockSpec(memory_space=pl.ANY)
    return pl.pallas_call(
        functools.partial(exchange_kernel, n, n_dev),
        out_shape=(
            jax.ShapeDtypeStruct(meta.shape, meta.dtype),
            jax.ShapeDtypeStruct(rows.shape, rows.dtype),
        ),
        in_specs=[anyspec, anyspec],
        out_specs=(anyspec, anyspec),
        scratch_shapes=[
            pltpu.SemaphoreType.DMA((2, n)),
            pltpu.SemaphoreType.DMA((2, n)),
            pltpu.SemaphoreType.DMA((2,)),
        ],
        compiler_params=pltpu.CompilerParams(collective_id=1, has_side_effects=True),
    )(meta, rows)


GROUP = 8
NEAR = 32
FAR = 16
FWD = 8
WINDOW = 256
BLOCKS = 3
CHUNK = 512
EARLY = 8
LATE = 12


def near_row(k):
    return k * NEAR + (k // EARLY) * 128 + (k // LATE) * 128


def far_row(k):
    return 256 + k * FAR + (k // EARLY) * 128


def relay_kernel(n_grp, n_dev, block_rows, fm_ref, slots_ref, pmeta_ref, chosen_ref,
                 rejected_ref, rows_out, packed_out, where_out, slot_out, head_out, flag_out,
                 rin, fin, fm_in, pin, pmeta_in, fwd, fwd_meta, fmeta_in, picks, scales, packed,
                 fm_sems, near_sems, far_sems, piece_sems, pm_sems, fwd_sems, fwdm_sems,
                 own_sems, save_sems, pack_sems):
    g = lax.axis_index("grp")
    v = lax.axis_index("dev")
    hd = n_dev // 2
    local_n = n_grp * hd
    half = v // hd
    u = lax.rem(v, hd)
    me = g * n_dev + v
    n = n_grp * n_dev
    pieces = n_grp + 1
    direct = local_n * (NEAR + FAR)
    far_base = local_n * NEAR
    other = 1 - half
    width = slots_ref.shape[1]
    f32 = jnp.float32

    def coord(t):
        return (t // n_dev, lax.rem(t, n_dev))

    barrier = pltpu.get_barrier_semaphore()

    def greet(k, c):
        pl.semaphore_signal(
            barrier, inc=1, device_id=coord(lax.rem(me + k, n)), device_id_type=MESH
        )
        return c

    lax.fori_loop(1, n, greet, 0)
    own = [
        pltpu.make_async_copy(fm_ref.at[me], fm_in.at[0], own_sems.at[0]),
        pltpu.make_async_copy(
            slots_ref.at[pl.ds(0, NEAR)], rin.at[pl.ds(0, NEAR)], own_sems.at[1]
        ),
    ]
    for cp in own:
        cp.start()
    pl.semaphore_wait(barrier, n - 1)

    def remote(src, dst, send_sem, recv_sem, to):
        return pltpu.make_async_remote_copy(
            src_ref=src, dst_ref=dst, send_sem=send_sem, recv_sem=recv_sem,
            device_id=to, device_id_type=MESH,
        )

    def partner(k, side):
        return lax.rem(g + k // hd, n_grp), side * hd + lax.rem(u + lax.rem(k, hd), hd)

    def piece_target(q):
        if q < n_grp:
            return (lax.rem(g + q, n_grp), other * hd + u)
        return (g, other * hd + lax.rem(u + hd // 2, hd))

    piece_copies = []
    for q in range(pieces):
        to = piece_target(q)
        piece_copies.append(
            remote(slots_ref.at[pl.ds(direct + q * GROUP, GROUP)], pin.at[q],
                   piece_sems.at[0, q], piece_sems.at[1, q], to)
        )
        piece_copies.append(
            remote(pmeta_ref.at[q], pmeta_in.at[q], pm_sems.at[0, q], pm_sems.at[1, q], to)
        )
    for cp in piece_copies:
        cp.start()

    def fm_copy(r):
        side = lax.rem(half + r // local_n, 2)
        tg, tv = partner(lax.rem(r, local_n), side)
        return remote(fm_ref.at[tg * n_dev + tv], fm_in.at[r], fm_sems.at[0, r],
                      fm_sems.at[1, r], (tg, tv))

    def near_copy(k):
        return remote(
            slots_ref.at[pl.ds(k * NEAR, NEAR)], rin.at[pl.ds(near_row(k), NEAR)],
            near_sems.at[0, k], near_sems.at[1, k], partner(k, half),
        )

    def far_copy(k):
        return remote(
            slots_ref.at[pl.ds(far_base + k * FAR, FAR)], rin.at[pl.ds(far_row(k), FAR)],
            far_sems.at[0, k], far_sems.at[1, k], partner(k, other),
        )

    def fwd_copies(k):
        to = partner(k, half)
        return [
            remote(fwd.at[k], fin.at[k], fwd_sems.at[0, k], fwd_sems.at[1, k], to),
            remote(fwd_meta.at[k], fmeta_in.at[k], fwdm_sems.at[0, k], fwdm_sems.at[1, k], to),
        ]

    def send_fm(r, c):
        fm_copy(r).start()
        return c

    lax.fori_loop(1, n, send_fm, 0)
    far_copy(0).start()

    def send_both(k, c):
        far_copy(k).start()
        near_copy(k).start()
        return c

    lax.fori_loop(1, local_n, send_both, 0)

    for cp in piece_copies:
        cp.wait_recv()
    count = pieces * GROUP
    marks = pmeta_in[...].reshape(count, 128)
    used = marks[:, 0:1] > 0.0
    dst_g = marks[:, 1:2].astype(jnp.int32)
    dst_u = marks[:, 2:3].astype(jnp.int32)
    dst = ((dst_g - g) & (n_grp - 1)) * hd + ((dst_u - u) & (hd - 1))
    lane = lax.broadcasted_iota(jnp.int32, (count, 128), 1)
    hot = jnp.where((lane == dst) & used, 1.0, 0.0)
    row_i = lax.broadcasted_iota(jnp.int32, (count, count), 0)
    col_i = lax.broadcasted_iota(jnp.int32, (count, count), 1)
    earlier = jnp.where(row_i > col_i, 1.0, 0.0)
    before = jnp.dot(earlier, hot, preferred_element_type=f32)
    rank = jnp.sum(before * hot, axis=1, keepdims=True).astype(jnp.int32)
    slot = jnp.where(used & (rank < FWD), dst * FWD + rank, -1)
    place = jnp.where(lane == slot, 1.0, 0.0)
    contract = (((0,), (0,)), ((), ()))
    rows_rows = (((1,), (1,)), ((), ()))

    def gather(c, carry):
        cols = pl.ds(pl.multiple_of(c * CHUNK, CHUNK), CHUNK)
        rows = pin[:, :, cols].astype(f32).reshape(count, CHUNK)
        out = lax.dot_general(place, rows, contract, preferred_element_type=f32)
        out = out.reshape(local_n, FWD, CHUNK).astype(jnp.bfloat16)
        fwd[:, :, cols] = out
        fin[0, :, cols] = out[0]
        return carry

    lax.fori_loop(0, width // CHUNK, gather, 0)
    out_meta = lax.dot_general(place, marks, contract, preferred_element_type=f32)
    out_meta = out_meta.reshape(local_n, FWD, 128)
    fwd_meta[...] = out_meta
    fmeta_in[0] = out_meta[0]

    def send_fwd(k, c):
        for cp in fwd_copies(k):
            cp.start()
        return c

    lax.fori_loop(1, local_n, send_fwd, 0)

    def wait_fm(r, c):
        cp = fm_copy(r)
        cp.wait_send()
        cp.wait_recv()
        return c

    own[0].wait()
    lax.fori_loop(1, n, wait_fm, 0)

    def source(r):
        a, b = (r & (local_n - 1)) // hd, r & (hd - 1)
        side = (half - r // local_n) & 1
        sg, su = (g - a) & (n_grp - 1), (u - b) & (hd - 1)
        return sg, su, sg * n_dev + side * hd + su

    reward = jnp.sum(fm_in[:, 0, :], axis=0, keepdims=True)
    pairs = chosen_ref.shape[0]
    pair_lane = lax.broadcasted_iota(jnp.int32, (pairs, 128), 1)
    sign = jnp.where(chosen_ref[...] == pair_lane, 1.0, 0.0) - jnp.where(
        rejected_ref[...] == pair_lane, 1.0, 0.0
    )
    margin = jnp.sum(sign * reward, axis=1, keepdims=True)
    push = -1.0 / (1.0 + jnp.exp(margin))
    reward_grad = jnp.sum(sign * push, axis=0, keepdims=True)
    eye0 = lax.broadcasted_iota(jnp.int32, (128, 128), 0)
    eye1 = lax.broadcasted_iota(jnp.int32, (128, 128), 1)
    grad_col = jnp.sum(jnp.where(eye0 == eye1, reward_grad, 0.0), axis=1, keepdims=True)
    src_lane = lax.broadcasted_iota(jnp.int32, (n, 128), 1)
    _, _, src = source(lax.broadcasted_iota(jnp.int32, (n, 128), 0))
    head = jnp.zeros((1, 128), f32)
    for j in range(4):
        part = jnp.where(src_lane == src * 4 + j, reward_grad, 0.0)
        coef = jnp.sum(part, axis=1, keepdims=True)
        head = head + jnp.sum(coef * fm_in[:, 4 + j, :], axis=0, keepdims=True)
    head_out[...] = jnp.broadcast_to(head, (8, 128))

    over = fm_in[:, 2, :]
    upper = jnp.where(eye0 < eye1, 1.0, 0.0)
    over_base = jnp.dot(over, upper, preferred_element_type=f32)
    here = lax.broadcasted_iota(jnp.int32, (local_n, n), 0)
    from_g, from_u, _ = source(lax.broadcasted_iota(jnp.int32, (local_n, n), 1))
    load = jnp.zeros((local_n, 128), f32)
    for q in range(pieces):
        part = jnp.floor((over_base + over - q + pieces - 0.5) * (1.0 / pieces)) - jnp.floor(
            (over_base - q + pieces - 0.5) * (1.0 / pieces)
        )
        if q < n_grp:
            at = ((from_g + q) & (n_grp - 1)) * hd + from_u
        else:
            at = from_g * hd + ((from_u + hd // 2) & (hd - 1))
        lands = jnp.where(at == here, 1.0, 0.0)
        load = load + jnp.dot(lands, part, preferred_element_type=f32)
    excess = jnp.maximum(
        jnp.max(jnp.max(load, axis=1, keepdims=True), axis=0, keepdims=True) - FWD,
        jnp.max(jnp.sum(over, axis=1, keepdims=True), axis=0, keepdims=True) - count,
    )

    def code_row(start, size):
        return jnp.sum(fm_in[pl.ds(start, size), 1, :], axis=0, keepdims=True)

    code_rows = [
        code_row(0, 4), code_row(4, 4), code_row(local_n, 8),
        code_row(8, 4), code_row(local_n + 8, 8), code_row(12, 4),
    ]
    tri = jnp.where(eye0 < eye1, 1.0, 0.0)
    sub = lax.broadcasted_iota(jnp.int32, (8, 128), 0)
    resp_id = eye0
    total = packed.shape[0]
    packed_id = lax.broadcasted_iota(jnp.int32, (total, 128), 0)

    def index_tile(i, target, resp, filled, worst, found):
        begin = sub * block_rows
        inside = (target >= begin) & (target < begin + block_rows) & (target >= 0)
        hot_b = jnp.where(inside, 1.0, 0.0)
        ahead = jnp.dot(hot_b, tri, preferred_element_type=f32) + filled
        rank_b = jnp.sum(hot_b * ahead, axis=0, keepdims=True).astype(jnp.int32)
        block = jnp.sum(jnp.where(inside, sub, 0), axis=0, keepdims=True)
        live = target >= 0
        ok = live & (rank_b < WINDOW)
        pos = jnp.where(ok, block * WINDOW + rank_b, -1)
        pick = jnp.where(packed_id == pos, 1.0, 0.0)
        picks[i] = pick.astype(jnp.bfloat16)
        scale = jnp.sum(jnp.where(resp_id == resp, grad_col, 0.0), axis=0, keepdims=True)
        scale = jnp.where(live, scale, 0.0)
        got = jnp.sum(pick * scale, axis=1, keepdims=True)
        marked = jnp.where(live, target + 1, 0)
        digits = jnp.where(sub == 0, marked >> 6, jnp.where(sub == 1, marked & 63, 0))
        found = found + lax.dot_general(
            digits.astype(f32), pick, rows_rows, preferred_element_type=f32
        )
        slot_out[i, 0:1, :] = (marked - 1).astype(f32)
        slot_out[i, 1:2, :] = scale
        filled = filled + jnp.sum(hot_b, axis=1, keepdims=True)
        worst = jnp.maximum(worst, jnp.max(filled, axis=0, keepdims=True))
        return filled, worst, found, got

    slot_out[...] = jnp.zeros_like(slot_out)
    filled = jnp.zeros((8, 1), f32)
    worst = jnp.zeros((1, 1), f32)
    found = jnp.zeros((8, total), f32)
    for i, row in enumerate(code_rows):
        code = row.astype(jnp.int32)
        filled, worst, found, got = index_tile(
            i, (code >> 7) - 1, code & 127, filled, worst, found
        )
        if i % 2 == 0:
            scales[i // 2] = got
        else:
            scales[i // 2] = scales[i // 2] + got

    def pack(seg, first):
        def col(c, carry):
            cols = pl.ds(pl.multiple_of(c * CHUNK, CHUNK), CHUNK)
            got = jnp.dot(picks[2 * seg], rin[pl.ds(seg * 256, 128), cols],
                          preferred_element_type=f32)
            got = got + jnp.dot(picks[2 * seg + 1], rin[pl.ds(seg * 256 + 128, 128), cols],
                                preferred_element_type=f32)
            got = (scales[seg] * got).astype(jnp.bfloat16)
            packed[:, cols] = got if first else packed[:, cols] + got
            return carry

        lax.fori_loop(0, width // CHUNK, col, 0)

    def save(i, src, start, size):
        return pltpu.make_async_copy(src, rows_out.at[pl.ds(start, size)], save_sems.at[i])

    def wait_far(k, c):
        cp = far_copy(k)
        cp.wait_send()
        cp.wait_recv()
        return c

    def wait_near(k, c):
        cp = near_copy(k)
        cp.wait_send()
        cp.wait_recv()
        return c

    own[1].wait()
    saves = [save(i, rin.at[pl.ds(i * 256, 256)], i * 256, 256) for i in range(3)]
    lax.fori_loop(1, EARLY, wait_near, 0)
    saves[0].start()
    pack(0, True)
    lax.fori_loop(0, EARLY, wait_far, 0)
    lax.fori_loop(EARLY, LATE, wait_near, 0)
    saves[1].start()
    pack(1, False)
    for cp in piece_copies:
        cp.wait_send()
    lax.fori_loop(EARLY, local_n, wait_far, 0)
    lax.fori_loop(LATE, local_n, wait_near, 0)
    saves[2].start()
    pack(2, False)

    def wait_fwd(k, c):
        for cp in fwd_copies(k):
            cp.wait_send()
            cp.wait_recv()
        return c

    lax.fori_loop(1, local_n, wait_fwd, 0)
    fmeta = fmeta_in[...].reshape(128, 128)
    pick_rows = jnp.where(
        lax.broadcasted_iota(jnp.int32, (8, 128), 0)
        == lax.broadcasted_iota(jnp.int32, (8, 128), 1), 1.0, 0.0
    )
    meta_rows = lax.dot_general(pick_rows, fmeta, rows_rows, preferred_element_type=f32)
    meta_rows = meta_rows.astype(jnp.int32)
    target = meta_rows[4:5] * 64 + meta_rows[5:6] - 1
    filled, worst, found, got = index_tile(6, target, meta_rows[3:4], filled, worst, found)
    scales[3] = got

    def pack_out(c):
        cols = pl.ds(c * CHUNK, CHUNK)
        return pltpu.make_async_copy(packed.at[:, cols], packed_out.at[:, cols], pack_sems.at[c])

    for c in range(width // CHUNK):
        cols = pl.ds(c * CHUNK, CHUNK)
        rows = fin[:, :, cols].astype(f32).reshape(128, CHUNK)
        got = jnp.dot(picks[6].astype(f32), rows, preferred_element_type=f32)
        packed[:, cols] = packed[:, cols] + (scales[3] * got).astype(jnp.bfloat16)
        pack_out(c).start()
    fwd_save = []
    for k in range(local_n):
        fwd_save.append(save(3 + k, fin.at[k], direct + k * FWD, FWD))
        fwd_save[-1].start()
    where_out[...] = found[0:1] * 64.0 + found[1:2] - 1.0 + jnp.zeros((8, total), f32)
    flag_out[0:1, :] = jnp.broadcast_to(excess, (1, 128))
    flag_out[1:8, :] = jnp.broadcast_to(worst - WINDOW, (7, 128))
    for cp in saves + fwd_save:
        cp.wait()
    for c in range(width // CHUNK):
        pack_out(c).wait()


def relay_exchange(fm, slots, pmeta, chosen, rejected, n_grp, n_dev, block_rows):
    n = n_grp * n_dev
    local_n = n // 2
    width = slots.shape[1]
    pieces = n_grp + 1
    direct = local_n * (NEAR + FAR)
    rows = direct + local_n * FWD
    total = BLOCKS * WINDOW
    anyspec = pl.BlockSpec(memory_space=pl.ANY)
    vmem = pl.BlockSpec(memory_space=pltpu.VMEM)
    sem = pltpu.SemaphoreType.DMA
    bf16, f32 = jnp.bfloat16, jnp.float32
    return pl.pallas_call(
        functools.partial(relay_kernel, n_grp, n_dev, block_rows),
        out_shape=(
            jax.ShapeDtypeStruct((rows, width), bf16),
            jax.ShapeDtypeStruct((total, width), bf16),
            jax.ShapeDtypeStruct((8, total), f32),
            jax.ShapeDtypeStruct((rows // 128, 8, 128), f32),
            jax.ShapeDtypeStruct((8, 128), f32),
            jax.ShapeDtypeStruct((8, 128), f32),
        ),
        in_specs=[anyspec, anyspec, anyspec, vmem, vmem],
        out_specs=(anyspec, anyspec, vmem, vmem, vmem, vmem),
        scratch_shapes=[
            pltpu.VMEM((direct, width), bf16),
            pltpu.VMEM((local_n, FWD, width), bf16),
            pltpu.VMEM((n, 8, 128), f32),
            pltpu.VMEM((pieces, GROUP, width), bf16),
            pltpu.VMEM((pieces, GROUP, 128), f32),
            pltpu.VMEM((local_n, FWD, width), bf16),
            pltpu.VMEM((local_n, FWD, 128), f32),
            pltpu.VMEM((local_n, FWD, 128), f32),
            pltpu.VMEM((rows // 128, total, 128), bf16),
            pltpu.VMEM((4, total, 1), f32),
            pltpu.VMEM((total, width), bf16),
            sem((2, n)),
            sem((2, local_n)),
            sem((2, local_n)),
            sem((2, pieces)),
            sem((2, pieces)),
            sem((2, local_n)),
            sem((2, local_n)),
            sem((2,)),
            sem((3 + local_n,)),
            sem((width // CHUNK,)),
        ],
        compiler_params=pltpu.CompilerParams(
            collective_id=0, has_side_effects=True, vmem_limit_bytes=56 * 1024 * 1024
        ),
    )(fm, slots, pmeta, chosen, rejected)


def place_kernel(where_ref, packed_ref, out_ref, src, onehot, outbuf, in_sems, out_sems):
    total, width = packed_ref.shape
    shard_rows = out_ref.shape[0]
    block_rows = shard_rows // BLOCKS
    padded = -(-block_rows // 16) * 16
    chunks = width // CHUNK
    slots = outbuf.shape[0]

    def fetch(c):
        return pltpu.make_async_copy(
            packed_ref.at[:, pl.ds(c * CHUNK, CHUNK)], src.at[c], in_sems.at[c]
        )

    def put(b, c, slot):
        return pltpu.make_async_copy(
            outbuf.at[slot, pl.ds(0, block_rows)],
            out_ref.at[pl.ds(b * block_rows, block_rows), pl.ds(c * CHUNK, CHUNK)],
            out_sems.at[slot],
        )

    for c in range(chunks):
        fetch(c).start()
    for b in range(BLOCKS):
        row_id = lax.broadcasted_iota(jnp.int32, (padded, WINDOW), 0) + b * block_rows
        target = where_ref[0:1, pl.ds(b * WINDOW, WINDOW)].astype(jnp.int32)
        onehot[...] = jnp.where(row_id == target, 1.0, 0.0).astype(jnp.bfloat16)
        for c in range(chunks):
            step = b * chunks + c
            if b == 0:
                fetch(c).wait()
            if step >= slots:
                put((step - slots) // chunks, (step - slots) % chunks, step % slots).wait()
            outbuf[step % slots] = jnp.dot(
                onehot[...], src[c, pl.ds(b * WINDOW, WINDOW), :],
                preferred_element_type=jnp.float32,
            ).astype(jnp.bfloat16)
            put(b, c, step % slots).start()
    steps = BLOCKS * chunks
    for step in range(steps - slots, steps):
        put(step // chunks, step % chunks, step % slots).wait()


def place_packed(shard_rows, where, packed):
    total, width = packed.shape
    chunks = width // CHUNK
    padded = -(-(shard_rows // BLOCKS) // 16) * 16
    vmem = pl.BlockSpec(memory_space=pltpu.VMEM)
    anyspec = pl.BlockSpec(memory_space=pl.ANY)
    return pl.pallas_call(
        place_kernel,
        out_shape=jax.ShapeDtypeStruct((shard_rows, width), packed.dtype),
        in_specs=[vmem, anyspec],
        out_specs=anyspec,
        scratch_shapes=[
            pltpu.VMEM((chunks, total, CHUNK), jnp.bfloat16),
            pltpu.VMEM((padded, WINDOW), jnp.bfloat16),
            pltpu.VMEM((4, padded, CHUNK), jnp.bfloat16),
            pltpu.SemaphoreType.DMA((chunks,)),
            pltpu.SemaphoreType.DMA((4,)),
        ],
        compiler_params=pltpu.CompilerParams(vmem_limit_bytes=48 * 1024 * 1024),
    )(where, packed)


def local(token_ids, sensitivity, last_hidden, lengths, norm_gain, reward_head,
          chosen_index, rejected_index, shard_owner):
    args = (token_ids, sensitivity, last_hidden, lengths, norm_gain, reward_head,
            chosen_index, rejected_index, shard_owner)
    resp_local, block_len = token_ids.shape
    devices = shard_owner.shape[0]
    n_grp, n_dev = lax.axis_size("grp"), lax.axis_size("dev")
    capacity = max(2, (2 * resp_local * block_len + devices - 1) // devices)
    shard_rows, width = VOCAB // devices, sensitivity.shape[2]
    if (capacity == NEAR and devices == 32 and n_grp in (1, 2, 4, 8) and n_dev % 4 == 0
            and resp_local == 4 and shard_rows % (8 * BLOCKS) == 0 and shard_rows < 64 * 250
            and width % CHUNK == 0 and width // devices <= 128):
        return relay_local(*args)
    prep = prepare(*args)
    return plain_finish(prep, n_dev)


def prepare(token_ids, sensitivity, last_hidden, lengths, norm_gain, reward_head,
            chosen_index, rejected_index, shard_owner):
    resp_local, block_len = token_ids.shape
    width = sensitivity.shape[2]
    tok_local = resp_local * block_len
    devices = shard_owner.shape[0]
    shard_rows = VOCAB // devices
    capacity = max(2, (2 * tok_local + devices - 1) // devices)
    hidden = last_hidden.astype(jnp.float32)
    normed = (
        hidden / jnp.sqrt(jnp.mean(hidden * hidden, axis=-1, keepdims=True) + 1e-05) * norm_gain
    )
    own_reward = jnp.sum(normed * reward_head, axis=-1)

    positions = jnp.arange(block_len, dtype=jnp.int32)
    live = (positions[None, :] < lengths[:, None]).reshape(tok_local)
    ids = token_ids.reshape(tok_local)
    shard_of = ids // shard_rows
    offset = ids - shard_of * shard_rows
    shard_hot = shard_of[:, None] == jnp.arange(devices, dtype=jnp.int32)[None, :]
    owner = jnp.sum(jnp.where(shard_hot, shard_owner[None, :], 0), axis=1)
    owner_hot = (owner[:, None] == jnp.arange(devices, dtype=jnp.int32)[None, :]) & live[:, None]
    live_hot = owner_hot.astype(jnp.bfloat16)
    token_pos = jnp.arange(tok_local, dtype=jnp.int32)
    earlier = (token_pos[:, None] > token_pos[None, :]).astype(jnp.bfloat16)
    before = jnp.dot(earlier, live_hot, preferred_element_type=jnp.float32)
    rank = jnp.sum(before * live_hot.astype(jnp.float32), axis=1).astype(jnp.int32)
    counts = jnp.sum(owner_hot.astype(jnp.int32), axis=0)
    return dict(
        sens=sensitivity.reshape(tok_local, width), normed=normed, own_reward=own_reward,
        live=live, offset=offset, owner=owner, rank=rank, counts=counts,
        owner_hot=owner_hot, resp=token_pos // block_len, capacity=capacity,
        chosen_index=chosen_index, rejected_index=rejected_index, devices=devices,
        shard_rows=shard_rows, resp_local=resp_local, width=width, tok_local=tok_local,
    )


def lane_pad(a, lanes):
    return jnp.pad(a, ((0, 0), (0, lanes - a.shape[1])))[:, None, :]


def reward_grads(p, reward):
    responses = p["devices"] * p["resp_local"]
    all_resp = jnp.arange(responses, dtype=jnp.int32)
    sign_table = (p["chosen_index"][:, None] == all_resp[None, :]).astype(jnp.float32) - (
        p["rejected_index"][:, None] == all_resp[None, :]
    ).astype(jnp.float32)
    margin = jnp.sum(sign_table * reward[None, :], axis=1)
    push = -jax.nn.sigmoid(-margin)
    return jnp.sum(sign_table * push[:, None], axis=0)


def place_all(shard_rows, rows, targets, scale):
    scaled = (scale[:, None] * rows).astype(jnp.bfloat16)
    placing = (targets[None, :] == jnp.arange(shard_rows, dtype=jnp.int32)[:, None]).astype(
        jnp.bfloat16
    )
    return jnp.dot(placing, scaled, preferred_element_type=jnp.float32).astype(jnp.bfloat16)


def plain_finish(p, n_dev):
    devices, capacity, resp_local = p["devices"], p["capacity"], p["resp_local"]
    width = p["width"]
    cols = width // devices
    responses = devices * resp_local
    lanes = -(-max(cols, capacity, resp_local) // 128) * 128
    slot = jnp.where(p["live"], p["owner"] * capacity + p["rank"], -1)
    slot_match = slot[None, :] == jnp.arange(devices * capacity, dtype=jnp.int32)[:, None]
    outgoing = jnp.dot(
        slot_match.astype(jnp.bfloat16), p["sens"], preferred_element_type=jnp.float32
    ).astype(jnp.bfloat16)
    code = (p["offset"] + 1) * resp_local + p["resp"]
    codes = jnp.sum(jnp.where(slot_match, code[None, :], 0), axis=1)
    codes = codes.reshape(devices, capacity)
    target_out = codes // resp_local - 1
    resp_out = codes - codes // resp_local * resp_local
    normed_blocks = p["normed"].reshape(resp_local, devices, cols).transpose(1, 0, 2)
    meta = jnp.concatenate(
        [
            lane_pad(target_out.astype(jnp.float32), lanes),
            lane_pad(resp_out.astype(jnp.float32), lanes),
            lane_pad(jnp.broadcast_to(p["own_reward"][None, :], (devices, resp_local)), lanes),
            jnp.zeros((devices, 1, lanes), jnp.float32),
            jnp.pad(normed_blocks, ((0, 0), (0, 0), (0, lanes - cols))),
        ],
        axis=1,
    )
    extra = -meta.shape[1] % 8
    meta = jnp.pad(meta, ((0, 0), (0, extra), (0, 0)))
    meta_in, arrived = exchange(
        meta, outgoing.reshape(devices, capacity, width), devices, n_dev
    )
    targets = meta_in[:, 0, :capacity].astype(jnp.int32).reshape(devices * capacity)
    resp_in = meta_in[:, 1, :capacity].astype(jnp.int32)
    reward = meta_in[:, 2, :resp_local].reshape(responses)
    normed_in = meta_in[:, 4 : 4 + resp_local, :cols]
    reward_grad = reward_grads(p, reward).reshape(devices, resp_local)
    head_grad = jnp.sum(reward_grad[:, :, None] * normed_in, axis=(0, 1))
    resp_hot = resp_in[:, :, None] == jnp.arange(resp_local, dtype=jnp.int32)[None, None, :]
    scale = jnp.sum(jnp.where(resp_hot, reward_grad[:, None, :], 0.0), axis=2)
    total = devices * capacity
    owned = place_all(
        p["shard_rows"], arrived.reshape(total, width), targets, scale.reshape(total)
    )
    return owned, head_grad


def relay_local(*args):
    n_grp, n_dev = lax.axis_size("grp"), lax.axis_size("dev")
    p = prepare(*args)
    devices, resp_local, width = p["devices"], p["resp_local"], p["width"]
    hd = n_dev // 2
    local_n = devices // 2
    pieces = n_grp + 1
    cols = width // devices
    g, v = lax.axis_index("grp"), lax.axis_index("dev")
    half = v // hd
    u = v % hd
    me = g * n_dev + v
    owner, rank, live = p["owner"], p["rank"], p["live"]
    owner_g, owner_v = owner // n_dev, owner % n_dev
    owner_u = owner_v % hd
    away = (owner_g - g) % n_grp * hd + (owner_u - u) % hd
    near = owner_v // hd == half
    dev_ids = jnp.arange(devices, dtype=jnp.int32)
    dev_far = dev_ids % n_dev // hd != half
    over = jnp.where(dev_far, jnp.maximum(p["counts"] - FAR, 0), 0)
    over_base = jnp.sum(jnp.where(dev_ids[None, :] < dev_ids[:, None], over[None, :], 0), axis=1)
    j = jnp.sum(jnp.where(p["owner_hot"], over_base[None, :], 0), axis=1) + rank - FAR
    far_start = local_n * NEAR
    piece_start = far_start + local_n * FAR
    slots = piece_start + pieces * GROUP
    piece_slot = jnp.where(
        j < pieces * GROUP, piece_start + j % pieces * GROUP + j // pieces, -1
    )
    slot = jnp.where(
        near,
        away * NEAR + rank,
        jnp.where(rank < FAR, far_start + away * FAR + rank, piece_slot),
    )
    slot = jnp.where(live, slot, -1)
    slot_match = slot[None, :] == jnp.arange(slots, dtype=jnp.int32)[:, None]
    outgoing = jnp.dot(
        slot_match.astype(jnp.bfloat16), p["sens"], preferred_element_type=jnp.float32
    ).astype(jnp.bfloat16)
    code = (p["offset"] + 1) * 128 + me * resp_local + p["resp"]
    lane_at = jnp.where(near, away % 4 * NEAR, away % 8 * FAR) + rank
    shown = live & (near | (rank < FAR))
    direct = jnp.where(shown, owner * 128 + lane_at, -1)
    direct_match = direct[None, :] == jnp.arange(devices * 128, dtype=jnp.int32)[:, None]
    codes = jnp.sum(jnp.where(direct_match, code[None, :], 0), axis=1).reshape(devices, 1, 128)
    piece_match = slot_match[piece_start:]
    piece_code = jnp.sum(jnp.where(piece_match, code[None, :], 0), axis=1)
    piece_owner = jnp.sum(
        jnp.where(piece_match, (owner_g * hd + owner_u)[None, :], 0), axis=1
    )
    piece_target = piece_code // 128
    lane = jnp.arange(128, dtype=jnp.int32)[None, :]
    pmeta = jnp.zeros((pieces * GROUP, 128), jnp.int32)
    for i, col in enumerate(
        (
            (piece_code > 0).astype(jnp.int32),
            piece_owner // hd,
            piece_owner % hd,
            piece_code % 128,
            piece_target // 64,
            piece_target % 64,
        )
    ):
        pmeta = jnp.where(lane == i, col[:, None], pmeta)
    pmeta = pmeta.astype(jnp.float32).reshape(pieces, GROUP, 128)
    normed_blocks = p["normed"].reshape(resp_local, devices, cols).transpose(1, 0, 2)
    reward_lane = jnp.arange(128, dtype=jnp.int32)[None, :] - me * resp_local
    reward_row = jnp.sum(
        jnp.where(
            reward_lane == jnp.arange(resp_local, dtype=jnp.int32)[:, None],
            p["own_reward"][:, None], 0.0,
        ),
        axis=0,
    )
    fm = jnp.concatenate(
        [
            jnp.broadcast_to(reward_row[None, None, :], (devices, 1, 128)),
            codes.astype(jnp.float32),
            lane_pad(jnp.broadcast_to(over.astype(jnp.float32)[None, :], (devices, devices)), 128),
            jnp.zeros((devices, 1, 128), jnp.float32),
            jnp.pad(normed_blocks, ((0, 0), (0, 4 - resp_local), (0, 128 - cols))),
        ],
        axis=1,
    )
    rows_in, packed, where, slot_info, head, flag = relay_exchange(
        fm, outgoing, pmeta, p["chosen_index"][:, None], p["rejected_index"][:, None],
        n_grp, n_dev, p["shard_rows"] // BLOCKS,
    )

    def relayed(operands):
        rows, packed, where, slot_info, flag = operands

        def spread(o):
            return place_all(
                p["shard_rows"], o[0], o[3][:, 0].reshape(-1).astype(jnp.int32),
                o[3][:, 1].reshape(-1),
            )

        return lax.cond(
            flag[1, 0] <= 0.0,
            lambda o: place_packed(p["shard_rows"], o[2], o[1]),
            spread,
            (rows, packed, where, slot_info),
        )

    owned = lax.cond(
        flag[0, 0] <= 0.0,
        relayed,
        lambda operands: plain_finish(p, n_dev)[0],
        (rows_in, packed, where, slot_info, flag),
    )
    return owned, head[0, :cols]


def solution(mesh):
    placed = (
        P(("grp", "dev"), None),
        P(("grp", "dev"), None, None),
        P(("grp", "dev"), None),
        P(("grp", "dev")),
        P(),
        P(),
        P(),
        P(),
        P(),
    )
    return jax.shard_map(
        local,
        mesh=mesh,
        in_specs=placed,
        out_specs=(P(("grp", "dev"), None), P(("grp", "dev"))),
        check_vma=False,
    )
```

```python
import functools

import jax
import jax.numpy as jnp
from jax import lax
from jax.experimental import pallas as pl
from jax.experimental.pallas import tpu as pltpu
from jax.sharding import PartitionSpec as P

VOCAB = 128256
MESH = pl.DeviceIdType.MESH


def exchange_kernel(n, n_dev, meta_ref, rows_ref, meta_out, rows_out, send_sem, recv_sem, own_sem):
    me = lax.axis_index("grp") * n_dev + lax.axis_index("dev")

    def coord(t):
        return (t // n_dev, lax.rem(t, n_dev))

    barrier = pltpu.get_barrier_semaphore()

    def greet(k, c):
        t = lax.rem(me + k, n)
        pl.semaphore_signal(barrier, inc=1, device_id=coord(t), device_id_type=MESH)
        return c

    lax.fori_loop(1, n, greet, 0)
    own = [
        pltpu.make_async_copy(src.at[me], dst.at[me], own_sem.at[i])
        for i, (src, dst) in enumerate(((meta_ref, meta_out), (rows_ref, rows_out)))
    ]
    for c in own:
        c.start()
    pl.semaphore_wait(barrier, n - 1)

    def copies(src_block, dst_block, to):
        return [
            pltpu.make_async_remote_copy(
                src_ref=src.at[src_block],
                dst_ref=dst.at[dst_block],
                send_sem=send_sem.at[i, src_block],
                recv_sem=recv_sem.at[i, dst_block],
                device_id=coord(to),
                device_id_type=MESH,
            )
            for i, (src, dst) in enumerate(((meta_ref, meta_out), (rows_ref, rows_out)))
        ]

    def send(k, c):
        t = lax.rem(me + k, n)
        for cp in copies(t, me, t):
            cp.start()
        return c

    lax.fori_loop(1, n, send, 0)

    def finish(k, c):
        t = lax.rem(me + k, n)
        for cp in copies(t, me, t):
            cp.wait_send()
        s = lax.rem(me + n - k, n)
        for cp in copies(s, s, s):
            cp.wait_recv()
        return c

    lax.fori_loop(1, n, finish, 0)
    for c in own:
        c.wait()


def exchange(meta, rows, n, n_dev):
    anyspec = pl.BlockSpec(memory_space=pl.ANY)
    return pl.pallas_call(
        functools.partial(exchange_kernel, n, n_dev),
        out_shape=(
            jax.ShapeDtypeStruct(meta.shape, meta.dtype),
            jax.ShapeDtypeStruct(rows.shape, rows.dtype),
        ),
        in_specs=[anyspec, anyspec],
        out_specs=(anyspec, anyspec),
        scratch_shapes=[
            pltpu.SemaphoreType.DMA((2, n)),
            pltpu.SemaphoreType.DMA((2, n)),
            pltpu.SemaphoreType.DMA((2,)),
        ],
        compiler_params=pltpu.CompilerParams(collective_id=1, has_side_effects=True),
    )(meta, rows)


GROUP = 8
NEAR = 32
FAR = 16
FWD = 8
AHEAD = 4
WINDOW = 256
BLOCKS = 3
CHUNK = 512
EARLY = 8
LATE = 12


def near_row(k):
    return k * NEAR + (k // EARLY) * 128 + (k // LATE) * 128


def far_row(k):
    return 256 + k * FAR + (k // EARLY) * 128


def log2(x):
    return x.bit_length() - 1


def relay_kernel(n_grp, n_dev, block_rows, ids_ref, sens_ref, hidden_ref, length_ref, gain_ref,
                 weight_ref, chosen_ref, rejected_ref, owner_ref,
                 rows_out, packed_out, where_out, slot_out, head_out, flag_out,
                 sens_v, select, slots_v, pout, fm_out, pmeta_out,
                 rin, fin, fm_in, pin, pmeta_in, fwd, fwd_meta, fmeta_in, picks, scales, packed,
                 sens_sems, fm_sems, near_sems, far_sems, piece_sems, pm_sems, fwd_sems,
                 fwdm_sems, save_sems, pack_sems):
    g = lax.axis_index("grp")
    v = lax.axis_index("dev")
    hd = n_dev // 2
    local_n = n_grp * hd
    half = v // hd
    u = lax.rem(v, hd)
    me = g * n_dev + v
    n = n_grp * n_dev
    pieces = n_grp + 1
    direct = local_n * (NEAR + FAR)
    far_base = local_n * NEAR
    other = 1 - half
    width = sens_ref.shape[1]
    f32 = jnp.float32
    chunks = width // CHUNK
    count = pieces * GROUP
    shard_rows = block_rows * BLOCKS
    i32 = jnp.int32
    rows_rows = (((1,), (1,)), ((), ()))

    def iota(rows, cols, axis):
        return lax.broadcasted_iota(i32, (rows, cols), axis)

    def coord(t):
        return (t // n_dev, lax.rem(t, n_dev))

    barrier = pltpu.get_barrier_semaphore()

    def greet(k, c):
        pl.semaphore_signal(
            barrier, inc=1, device_id=coord(lax.rem(me + k, n)), device_id_type=MESH
        )
        return c

    lax.fori_loop(1, n, greet, 0)
    def fetch(c):
        return pltpu.make_async_copy(
            sens_ref.at[:, pl.ds(c * CHUNK, CHUNK)], sens_v.at[c], sens_sems.at[c]
        )

    for c in range(chunks):
        fetch(c).start()

    eye0, eye1 = iota(128, 128, 0), iota(128, 128, 1)
    tri = jnp.where(eye0 < eye1, 1.0, 0.0)
    resp_local, block_len = ids_ref.shape
    resp_row, resp_pos = iota(resp_local, block_len, 0), iota(resp_local, block_len, 1)
    ids = ids_ref[...]
    length = jnp.zeros((resp_local, block_len), i32)
    for r in range(resp_local):
        length = jnp.where(resp_row == r, length_ref[r], length)
    live_all = resp_pos < length
    shard = jnp.floor((ids.astype(f32) + 0.5) * (1.0 / shard_rows)).astype(i32)
    above = ids - shard * shard_rows + 1
    owner_all = jnp.zeros((resp_local, block_len), i32)
    for k in range(n):
        owner_all = jnp.where(shard == k, owner_ref[k], owner_all)
    owner_g = owner_all >> log2(n_dev)
    owner_v = owner_all & (n_dev - 1)
    owner_u = owner_v & (hd - 1)
    near_all = (owner_v >> log2(hd)) == half
    away_all = (((owner_g - g) & (n_grp - 1)) << log2(hd)) + ((owner_u - u) & (hd - 1))
    dev_row = iota(n, 128, 0)
    filled_to = jnp.zeros((n, 1), f32)
    hots, ranks = [], []
    for r in range(resp_local):
        live = live_all[r : r + 1]
        hot = jnp.where((dev_row == owner_all[r : r + 1]) & live, 1.0, 0.0)
        ahead = jnp.dot(hot, tri, preferred_element_type=f32) + filled_to
        ranks.append(jnp.sum(hot * ahead, axis=0, keepdims=True))
        filled_to = filled_to + jnp.sum(hot, axis=1, keepdims=True)
        hots.append(hot)
    dev_far = ((dev_row & (n_dev - 1)) >> log2(hd)) != half
    over_out = jnp.where(dev_far, jnp.maximum(filled_to - FAR, 0.0), 0.0)
    lower = jnp.where(iota(n, n, 0) > iota(n, n, 1), 1.0, 0.0)
    base_out = jnp.dot(lower, over_out, preferred_element_type=f32)
    over_row = jnp.sum(
        jnp.where(dev_row == iota(n, 128, 1), over_out, 0.0), axis=0, keepdims=True
    )
    code_hi = jnp.zeros((n, 128), f32)
    code_lo = jnp.zeros((n, 128), f32)
    code_resp = jnp.zeros((n, 128), f32)
    piece_meta = jnp.zeros((count, 128), f32)
    for r in range(resp_local):
        live, near = live_all[r : r + 1], near_all[r : r + 1]
        away, rank = away_all[r : r + 1], ranks[r]
        place_j = jnp.sum(hots[r] * base_out, axis=0, keepdims=True) + rank - FAR
        level = jnp.floor((place_j + 0.5) * (1.0 / pieces))
        piece = direct + (place_j - pieces * level) * GROUP + level
        piece = jnp.where(place_j < count, piece, -1.0).astype(i32)
        rank = rank.astype(i32)
        slot = jnp.where(
            near,
            away * NEAR + rank,
            jnp.where(rank < FAR, far_base + away * FAR + rank, piece),
        )
        slot = jnp.where(live, slot, -1)
        select[:, pl.ds(r * 128, 128)] = jnp.where(
            iota(direct + 48, 128, 0) == slot, 1.0, 0.0
        ).astype(jnp.bfloat16)
        lane_at = jnp.where(near, (away & 3) * NEAR, (away & 7) * FAR) + rank
        shown = live & (near | (rank < FAR))
        at_hot = jnp.where(eye0 == jnp.where(shown, lane_at, -1), 1.0, 0.0)
        hi = (above[r : r + 1] >> 6).astype(f32)
        lo = (above[r : r + 1] & 63).astype(f32)
        resp = (iota(1, 128, 1) * 0 + (me * resp_local + r)).astype(f32)
        code_hi += lax.dot_general(hots[r] * hi, at_hot, rows_rows, preferred_element_type=f32)
        code_lo += lax.dot_general(hots[r] * lo, at_hot, rows_rows, preferred_element_type=f32)
        code_resp += lax.dot_general(
            hots[r] * resp, at_hot, rows_rows, preferred_element_type=f32
        )
        feature = jnp.where(eye0 == 0, 1.0, 0.0)
        for i, row in (
            (1, owner_g[r : r + 1].astype(f32)), (2, owner_u[r : r + 1].astype(f32)),
            (3, resp), (4, hi), (5, lo),
        ):
            feature = jnp.where(eye0 == i, row, feature)
        in_piece = jnp.where(iota(count, 128, 0) + direct == slot, 1.0, 0.0)
        piece_meta += lax.dot_general(
            in_piece, feature, rows_rows, preferred_element_type=f32
        )
    pmeta_out[...] = piece_meta.reshape(pieces, GROUP, 128)

    hidden = hidden_ref[...].astype(f32)
    square = jnp.sum(hidden * hidden, axis=1, keepdims=True) * (1.0 / width)
    normed = hidden / jnp.sqrt(square + 1e-05) * gain_ref[...]
    own_reward = jnp.sum(normed * weight_ref[...], axis=1, keepdims=True)
    reward_row = jnp.sum(
        jnp.where(resp_pos == me * resp_local + resp_row, own_reward, 0.0),
        axis=0, keepdims=True,
    )
    fm_out[:, 0, :] = jnp.broadcast_to(reward_row, (n, 128))
    fm_out[:, 1, :] = (code_hi * 64.0 + code_lo) * 128.0 + code_resp
    fm_out[:, 2, :] = jnp.broadcast_to(over_row, (n, 128))
    fm_out[:, 3, :] = jnp.zeros((n, 128), f32)
    for d in range(n):
        fm_out[d, 4:8, :] = normed[:, d * 128 : (d + 1) * 128]
    fm_in[0] = fm_out[me]

    def build_far(c, carry):
        cols = pl.ds(pl.multiple_of(c * CHUNK, CHUNK), CHUNK)
        fetch(c).wait()
        got = jnp.dot(select[pl.ds(far_base, direct + 48 - far_base), :], sens_v[c],
                      preferred_element_type=f32)
        slots_v[pl.ds(far_base, direct - far_base), cols] = got[
            : direct - far_base
        ].astype(jnp.bfloat16)
        pout[:, :, cols] = got[direct - far_base : direct - far_base + count].reshape(
            pieces, GROUP, CHUNK
        ).astype(jnp.bfloat16)
        return carry

    lax.fori_loop(0, chunks, build_far, 0)
    pl.semaphore_wait(barrier, n - 1)

    def remote(src, dst, send_sem, recv_sem, to):
        return pltpu.make_async_remote_copy(
            src_ref=src, dst_ref=dst, send_sem=send_sem, recv_sem=recv_sem,
            device_id=to, device_id_type=MESH,
        )

    def partner(k, side):
        return lax.rem(g + k // hd, n_grp), side * hd + lax.rem(u + lax.rem(k, hd), hd)

    def piece_target(q):
        if q < n_grp:
            return (lax.rem(g + q, n_grp), other * hd + u)
        return (g, other * hd + lax.rem(u + hd // 2, hd))

    piece_copies = []
    for q in range(pieces):
        to = piece_target(q)
        piece_copies.append(
            remote(pout.at[q], pin.at[q],
                   piece_sems.at[0, q], piece_sems.at[1, q], to)
        )
        piece_copies.append(
            remote(pmeta_out.at[q], pmeta_in.at[q], pm_sems.at[0, q], pm_sems.at[1, q], to)
        )
    for cp in piece_copies:
        cp.start()

    def fm_copy(r):
        side = lax.rem(half + r // local_n, 2)
        tg, tv = partner(lax.rem(r, local_n), side)
        return remote(fm_out.at[tg * n_dev + tv], fm_in.at[r], fm_sems.at[0, r],
                      fm_sems.at[1, r], (tg, tv))

    def near_copy(k):
        return remote(
            slots_v.at[pl.ds(k * NEAR, NEAR)], rin.at[pl.ds(near_row(k), NEAR)],
            near_sems.at[0, k], near_sems.at[1, k], partner(k, half),
        )

    def far_copy(k):
        return remote(
            slots_v.at[pl.ds(far_base + k * FAR, FAR)], rin.at[pl.ds(far_row(k), FAR)],
            far_sems.at[0, k], far_sems.at[1, k], partner(k, other),
        )

    def fwd_copies(k):
        to = partner(k, half)
        return [
            remote(fwd.at[k], fin.at[k], fwd_sems.at[0, k], fwd_sems.at[1, k], to),
            remote(fwd_meta.at[k], fmeta_in.at[k], fwdm_sems.at[0, k], fwdm_sems.at[1, k], to),
        ]

    def send_fm(r, c):
        fm_copy(r).start()
        return c

    lax.fori_loop(1, n, send_fm, 0)

    def send_far(k, c):
        far_copy(k).start()
        return c

    def send_both(k, c):
        far_copy(k).start()
        near_copy(k).start()
        return c

    def send_near(k, c):
        near_copy(k).start()
        return c

    lax.fori_loop(0, AHEAD, send_far, 0)

    def build_near(c, carry):
        cols = pl.ds(pl.multiple_of(c * CHUNK, CHUNK), CHUNK)
        got = jnp.dot(select[pl.ds(0, far_base), :], sens_v[c],
                      preferred_element_type=f32).astype(jnp.bfloat16)
        slots_v[pl.ds(0, far_base), cols] = got
        rin[pl.ds(0, NEAR), cols] = got[:NEAR]
        return carry

    lax.fori_loop(0, chunks, build_near, 0)
    lax.fori_loop(1, AHEAD, send_near, 0)
    lax.fori_loop(AHEAD, local_n, send_both, 0)

    for cp in piece_copies:
        cp.wait_recv()
    marks = pmeta_in[...].reshape(count, 128)
    used = marks[:, 0:1] > 0.0
    dst_g = marks[:, 1:2].astype(jnp.int32)
    dst_u = marks[:, 2:3].astype(jnp.int32)
    dst = ((dst_g - g) & (n_grp - 1)) * hd + ((dst_u - u) & (hd - 1))
    lane = lax.broadcasted_iota(jnp.int32, (count, 128), 1)
    hot = jnp.where((lane == dst) & used, 1.0, 0.0)
    row_i = lax.broadcasted_iota(jnp.int32, (count, count), 0)
    col_i = lax.broadcasted_iota(jnp.int32, (count, count), 1)
    earlier = jnp.where(row_i > col_i, 1.0, 0.0)
    before = jnp.dot(earlier, hot, preferred_element_type=f32)
    rank = jnp.sum(before * hot, axis=1, keepdims=True).astype(jnp.int32)
    slot = jnp.where(used & (rank < FWD), dst * FWD + rank, -1)
    place = jnp.where(lane == slot, 1.0, 0.0)
    contract = (((0,), (0,)), ((), ()))

    def gather(c, carry):
        cols = pl.ds(pl.multiple_of(c * CHUNK, CHUNK), CHUNK)
        rows = pin[:, :, cols].astype(f32).reshape(count, CHUNK)
        out = lax.dot_general(place, rows, contract, preferred_element_type=f32)
        out = out.reshape(local_n, FWD, CHUNK).astype(jnp.bfloat16)
        fwd[:, :, cols] = out
        fin[0, :, cols] = out[0]
        return carry

    lax.fori_loop(0, width // CHUNK, gather, 0)
    out_meta = lax.dot_general(place, marks, contract, preferred_element_type=f32)
    out_meta = out_meta.reshape(local_n, FWD, 128)
    fwd_meta[...] = out_meta
    fmeta_in[0] = out_meta[0]

    def send_fwd(k, c):
        for cp in fwd_copies(k):
            cp.start()
        return c

    lax.fori_loop(1, local_n, send_fwd, 0)

    def wait_fm(r, c):
        cp = fm_copy(r)
        cp.wait_send()
        cp.wait_recv()
        return c

    lax.fori_loop(1, n, wait_fm, 0)

    def source(r):
        a, b = (r & (local_n - 1)) // hd, r & (hd - 1)
        side = (half - r // local_n) & 1
        sg, su = (g - a) & (n_grp - 1), (u - b) & (hd - 1)
        return sg, su, sg * n_dev + side * hd + su

    reward = jnp.sum(fm_in[:, 0, :], axis=0, keepdims=True)
    pairs = chosen_ref.shape[0]
    pair_row = iota(pairs, 1, 0)
    chosen = jnp.zeros((pairs, 1), i32)
    rejected = jnp.zeros((pairs, 1), i32)
    for k in range(pairs):
        chosen = jnp.where(pair_row == k, chosen_ref[k], chosen)
        rejected = jnp.where(pair_row == k, rejected_ref[k], rejected)
    pair_lane = iota(pairs, 128, 1)
    sign = jnp.where(chosen == pair_lane, 1.0, 0.0) - jnp.where(
        rejected == pair_lane, 1.0, 0.0
    )
    margin = jnp.sum(sign * reward, axis=1, keepdims=True)
    push = -1.0 / (1.0 + jnp.exp(margin))
    reward_grad = jnp.sum(sign * push, axis=0, keepdims=True)
    grad_col = jnp.sum(jnp.where(eye0 == eye1, reward_grad, 0.0), axis=1, keepdims=True)
    src_lane = lax.broadcasted_iota(jnp.int32, (n, 128), 1)
    _, _, src = source(lax.broadcasted_iota(jnp.int32, (n, 128), 0))
    head = jnp.zeros((1, 128), f32)
    for j in range(4):
        part = jnp.where(src_lane == src * 4 + j, reward_grad, 0.0)
        coef = jnp.sum(part, axis=1, keepdims=True)
        head = head + jnp.sum(coef * fm_in[:, 4 + j, :], axis=0, keepdims=True)
    head_out[...] = head

    over = fm_in[:, 2, :]
    over_base = jnp.dot(over, tri, preferred_element_type=f32)
    here = lax.broadcasted_iota(jnp.int32, (local_n, n), 0)
    from_g, from_u, _ = source(lax.broadcasted_iota(jnp.int32, (local_n, n), 1))
    load = jnp.zeros((local_n, 128), f32)
    for q in range(pieces):
        part = jnp.floor((over_base + over - q + pieces - 0.5) * (1.0 / pieces)) - jnp.floor(
            (over_base - q + pieces - 0.5) * (1.0 / pieces)
        )
        if q < n_grp:
            at = ((from_g + q) & (n_grp - 1)) * hd + from_u
        else:
            at = from_g * hd + ((from_u + hd // 2) & (hd - 1))
        lands = jnp.where(at == here, 1.0, 0.0)
        load = load + jnp.dot(lands, part, preferred_element_type=f32)
    excess = jnp.maximum(
        jnp.max(jnp.max(load, axis=1, keepdims=True), axis=0, keepdims=True) - FWD,
        jnp.max(jnp.sum(over, axis=1, keepdims=True), axis=0, keepdims=True) - count,
    )

    def code_row(start, size):
        return jnp.sum(fm_in[pl.ds(start, size), 1, :], axis=0, keepdims=True)

    code_rows = [
        code_row(0, 4), code_row(4, 4), code_row(local_n, 8),
        code_row(8, 4), code_row(local_n + 8, 8), code_row(12, 4),
    ]
    sub = lax.broadcasted_iota(jnp.int32, (8, 128), 0)
    resp_id = eye0
    total = packed.shape[0]
    packed_id = lax.broadcasted_iota(jnp.int32, (total, 128), 0)

    def index_tile(i, target, resp, filled, worst, found):
        begin = sub * block_rows
        inside = (target >= begin) & (target < begin + block_rows) & (target >= 0)
        hot_b = jnp.where(inside, 1.0, 0.0)
        ahead = jnp.dot(hot_b, tri, preferred_element_type=f32) + filled
        rank_b = jnp.sum(hot_b * ahead, axis=0, keepdims=True).astype(jnp.int32)
        block = jnp.sum(jnp.where(inside, sub, 0), axis=0, keepdims=True)
        live = target >= 0
        ok = live & (rank_b < WINDOW)
        pos = jnp.where(ok, block * WINDOW + rank_b, -1)
        pick = jnp.where(packed_id == pos, 1.0, 0.0)
        picks[i] = pick.astype(jnp.bfloat16)
        scale = jnp.sum(jnp.where(resp_id == resp, grad_col, 0.0), axis=0, keepdims=True)
        scale = jnp.where(live, scale, 0.0)
        got = jnp.sum(pick * scale, axis=1, keepdims=True)
        marked = jnp.where(live, target + 1, 0)
        digits = jnp.where(sub == 0, marked >> 6, jnp.where(sub == 1, marked & 63, 0))
        found = found + lax.dot_general(
            digits.astype(f32), pick, rows_rows, preferred_element_type=f32
        )
        slot_out[i, 0:1, :] = (marked - 1).astype(f32)
        slot_out[i, 1:2, :] = scale
        filled = filled + jnp.sum(hot_b, axis=1, keepdims=True)
        worst = jnp.maximum(worst, jnp.max(filled, axis=0, keepdims=True))
        return filled, worst, found, got

    slot_out[...] = jnp.zeros_like(slot_out)
    filled = jnp.zeros((8, 1), f32)
    worst = jnp.zeros((1, 1), f32)
    found = jnp.zeros((8, total), f32)
    for i, row in enumerate(code_rows):
        code = row.astype(jnp.int32)
        filled, worst, found, got = index_tile(
            i, (code >> 7) - 1, code & 127, filled, worst, found
        )
        if i % 2 == 0:
            scales[i // 2] = got
        else:
            scales[i // 2] = scales[i // 2] + got

    def pack(seg, first):
        def col(c, carry):
            cols = pl.ds(pl.multiple_of(c * CHUNK, CHUNK), CHUNK)
            got = jnp.dot(picks[2 * seg], rin[pl.ds(seg * 256, 128), cols],
                          preferred_element_type=f32)
            got = got + jnp.dot(picks[2 * seg + 1], rin[pl.ds(seg * 256 + 128, 128), cols],
                                preferred_element_type=f32)
            got = (scales[seg] * got).astype(jnp.bfloat16)
            packed[:, cols] = got if first else packed[:, cols] + got
            return carry

        lax.fori_loop(0, width // CHUNK, col, 0)

    def save(i, src, start, size):
        return pltpu.make_async_copy(src, rows_out.at[pl.ds(start, size)], save_sems.at[i])

    def wait_far(k, c):
        cp = far_copy(k)
        cp.wait_send()
        cp.wait_recv()
        return c

    def wait_near(k, c):
        cp = near_copy(k)
        cp.wait_send()
        cp.wait_recv()
        return c

    saves = [save(i, rin.at[pl.ds(i * 256, 256)], i * 256, 256) for i in range(3)]
    lax.fori_loop(1, EARLY, wait_near, 0)
    saves[0].start()
    pack(0, True)
    lax.fori_loop(0, EARLY, wait_far, 0)
    lax.fori_loop(EARLY, LATE, wait_near, 0)
    saves[1].start()
    pack(1, False)
    for cp in piece_copies:
        cp.wait_send()
    lax.fori_loop(EARLY, local_n, wait_far, 0)
    lax.fori_loop(LATE, local_n, wait_near, 0)
    saves[2].start()
    pack(2, False)

    def wait_fwd(k, c):
        for cp in fwd_copies(k):
            cp.wait_send()
            cp.wait_recv()
        return c

    lax.fori_loop(1, local_n, wait_fwd, 0)
    fmeta = fmeta_in[...].reshape(128, 128)
    pick_rows = jnp.where(
        lax.broadcasted_iota(jnp.int32, (8, 128), 0)
        == lax.broadcasted_iota(jnp.int32, (8, 128), 1), 1.0, 0.0
    )
    meta_rows = lax.dot_general(pick_rows, fmeta, rows_rows, preferred_element_type=f32)
    meta_rows = meta_rows.astype(jnp.int32)
    target = meta_rows[4:5] * 64 + meta_rows[5:6] - 1
    filled, worst, found, got = index_tile(6, target, meta_rows[3:4], filled, worst, found)
    scales[3] = got

    def pack_out(c):
        cols = pl.ds(c * CHUNK, CHUNK)
        return pltpu.make_async_copy(packed.at[:, cols], packed_out.at[:, cols], pack_sems.at[c])

    for c in range(width // CHUNK):
        cols = pl.ds(c * CHUNK, CHUNK)
        rows = fin[:, :, cols].astype(f32).reshape(128, CHUNK)
        got = jnp.dot(picks[6].astype(f32), rows, preferred_element_type=f32)
        packed[:, cols] = packed[:, cols] + (scales[3] * got).astype(jnp.bfloat16)
        pack_out(c).start()
    fwd_save = []
    for k in range(local_n):
        fwd_save.append(save(3 + k, fin.at[k], direct + k * FWD, FWD))
        fwd_save[-1].start()
    where_out[...] = found[0:1] * 64.0 + found[1:2] - 1.0 + jnp.zeros((8, total), f32)
    flag_out[0:1, :] = jnp.broadcast_to(excess, (1, 128))
    flag_out[1:8, :] = jnp.broadcast_to(worst - WINDOW, (7, 128))
    for cp in saves + fwd_save:
        cp.wait()
    for c in range(width // CHUNK):
        pack_out(c).wait()


def relay_exchange(args, n_grp, n_dev, block_rows):
    ids, sens, hidden, lengths, gain, weight, chosen, rejected, owner = args
    resp_local, block_len, width = sens.shape
    n = n_grp * n_dev
    local_n = n // 2
    pieces = n_grp + 1
    direct = local_n * (NEAR + FAR)
    rows = direct + local_n * FWD
    total = BLOCKS * WINDOW
    anyspec = pl.BlockSpec(memory_space=pl.ANY)
    vmem = pl.BlockSpec(memory_space=pltpu.VMEM)
    smem = pl.BlockSpec(memory_space=pltpu.SMEM)
    sem = pltpu.SemaphoreType.DMA
    bf16, f32 = jnp.bfloat16, jnp.float32
    return pl.pallas_call(
        functools.partial(relay_kernel, n_grp, n_dev, block_rows),
        out_shape=(
            jax.ShapeDtypeStruct((rows, width), bf16),
            jax.ShapeDtypeStruct((total, width), bf16),
            jax.ShapeDtypeStruct((8, total), f32),
            jax.ShapeDtypeStruct((rows // 128, 8, 128), f32),
            jax.ShapeDtypeStruct((1, 128), f32),
            jax.ShapeDtypeStruct((8, 128), f32),
        ),
        in_specs=[vmem, anyspec, vmem, smem, vmem, vmem, smem, smem, smem],
        out_specs=(anyspec, anyspec, vmem, vmem, vmem, vmem),
        scratch_shapes=[
            pltpu.VMEM((width // CHUNK, resp_local * block_len, CHUNK), bf16),
            pltpu.VMEM((direct + 48, resp_local * block_len), bf16),
            pltpu.VMEM((direct, width), bf16),
            pltpu.VMEM((pieces, GROUP, width), bf16),
            pltpu.VMEM((n, 8, 128), f32),
            pltpu.VMEM((pieces, GROUP, 128), f32),
            pltpu.VMEM((direct, width), bf16),
            pltpu.VMEM((local_n, FWD, width), bf16),
            pltpu.VMEM((n, 8, 128), f32),
            pltpu.VMEM((pieces, GROUP, width), bf16),
            pltpu.VMEM((pieces, GROUP, 128), f32),
            pltpu.VMEM((local_n, FWD, width), bf16),
            pltpu.VMEM((local_n, FWD, 128), f32),
            pltpu.VMEM((local_n, FWD, 128), f32),
            pltpu.VMEM((rows // 128, total, 128), bf16),
            pltpu.VMEM((4, total, 1), f32),
            pltpu.VMEM((total, width), bf16),
            sem((width // CHUNK,)),
            sem((2, n)),
            sem((2, local_n)),
            sem((2, local_n)),
            sem((2, pieces)),
            sem((2, pieces)),
            sem((2, local_n)),
            sem((2, local_n)),
            sem((3 + local_n,)),
            sem((width // CHUNK,)),
        ],
        compiler_params=pltpu.CompilerParams(
            collective_id=0, has_side_effects=True, vmem_limit_bytes=56 * 1024 * 1024
        ),
    )(ids, sens.reshape(-1, width), hidden, lengths, gain[None, :], weight[None, :], chosen,
      rejected, owner)


def place_kernel(where_ref, packed_ref, out_ref, src, onehot, outbuf, in_sems, out_sems):
    total, width = packed_ref.shape
    shard_rows = out_ref.shape[0]
    block_rows = shard_rows // BLOCKS
    padded = -(-block_rows // 16) * 16
    chunks = width // CHUNK
    slots = outbuf.shape[0]

    def fetch(c):
        return pltpu.make_async_copy(
            packed_ref.at[:, pl.ds(c * CHUNK, CHUNK)], src.at[c], in_sems.at[c]
        )

    def put(b, c, slot):
        return pltpu.make_async_copy(
            outbuf.at[slot, pl.ds(0, block_rows)],
            out_ref.at[pl.ds(b * block_rows, block_rows), pl.ds(c * CHUNK, CHUNK)],
            out_sems.at[slot],
        )

    for c in range(chunks):
        fetch(c).start()
    for b in range(BLOCKS):
        row_id = lax.broadcasted_iota(jnp.int32, (padded, WINDOW), 0) + b * block_rows
        target = where_ref[0:1, pl.ds(b * WINDOW, WINDOW)].astype(jnp.int32)
        onehot[...] = jnp.where(row_id == target, 1.0, 0.0).astype(jnp.bfloat16)
        for c in range(chunks):
            step = b * chunks + c
            if b == 0:
                fetch(c).wait()
            if step >= slots:
                put((step - slots) // chunks, (step - slots) % chunks, step % slots).wait()
            outbuf[step % slots] = jnp.dot(
                onehot[...], src[c, pl.ds(b * WINDOW, WINDOW), :],
                preferred_element_type=jnp.float32,
            ).astype(jnp.bfloat16)
            put(b, c, step % slots).start()
    steps = BLOCKS * chunks
    for step in range(steps - slots, steps):
        put(step // chunks, step % chunks, step % slots).wait()


def place_packed(shard_rows, where, packed):
    total, width = packed.shape
    chunks = width // CHUNK
    padded = -(-(shard_rows // BLOCKS) // 16) * 16
    vmem = pl.BlockSpec(memory_space=pltpu.VMEM)
    anyspec = pl.BlockSpec(memory_space=pl.ANY)
    return pl.pallas_call(
        place_kernel,
        out_shape=jax.ShapeDtypeStruct((shard_rows, width), packed.dtype),
        in_specs=[vmem, anyspec],
        out_specs=anyspec,
        scratch_shapes=[
            pltpu.VMEM((chunks, total, CHUNK), jnp.bfloat16),
            pltpu.VMEM((padded, WINDOW), jnp.bfloat16),
            pltpu.VMEM((4, padded, CHUNK), jnp.bfloat16),
            pltpu.SemaphoreType.DMA((chunks,)),
            pltpu.SemaphoreType.DMA((4,)),
        ],
        compiler_params=pltpu.CompilerParams(vmem_limit_bytes=48 * 1024 * 1024),
    )(where, packed)


def local(token_ids, sensitivity, last_hidden, lengths, norm_gain, reward_head,
          chosen_index, rejected_index, shard_owner):
    args = (token_ids, sensitivity, last_hidden, lengths, norm_gain, reward_head,
            chosen_index, rejected_index, shard_owner)
    resp_local, block_len = token_ids.shape
    devices = shard_owner.shape[0]
    n_grp, n_dev = lax.axis_size("grp"), lax.axis_size("dev")
    capacity = max(2, (2 * resp_local * block_len + devices - 1) // devices)
    shard_rows, width = VOCAB // devices, sensitivity.shape[2]
    if (capacity == NEAR and devices == 32 and n_grp in (1, 2, 4, 8) and n_dev % 4 == 0
            and resp_local == 4 and shard_rows % (8 * BLOCKS) == 0 and shard_rows < 64 * 250
            and width % CHUNK == 0 and width // devices == 128 and block_len == 128):
        return relay_local(*args)
    prep = prepare(*args)
    return plain_finish(prep, n_dev)


def prepare(token_ids, sensitivity, last_hidden, lengths, norm_gain, reward_head,
            chosen_index, rejected_index, shard_owner):
    resp_local, block_len = token_ids.shape
    width = sensitivity.shape[2]
    tok_local = resp_local * block_len
    devices = shard_owner.shape[0]
    shard_rows = VOCAB // devices
    capacity = max(2, (2 * tok_local + devices - 1) // devices)
    hidden = last_hidden.astype(jnp.float32)
    normed = (
        hidden / jnp.sqrt(jnp.mean(hidden * hidden, axis=-1, keepdims=True) + 1e-05) * norm_gain
    )
    own_reward = jnp.sum(normed * reward_head, axis=-1)

    positions = jnp.arange(block_len, dtype=jnp.int32)
    live = (positions[None, :] < lengths[:, None]).reshape(tok_local)
    ids = token_ids.reshape(tok_local)
    shard_of = ids // shard_rows
    offset = ids - shard_of * shard_rows
    shard_hot = shard_of[:, None] == jnp.arange(devices, dtype=jnp.int32)[None, :]
    owner = jnp.sum(jnp.where(shard_hot, shard_owner[None, :], 0), axis=1)
    owner_hot = (owner[:, None] == jnp.arange(devices, dtype=jnp.int32)[None, :]) & live[:, None]
    live_hot = owner_hot.astype(jnp.bfloat16)
    token_pos = jnp.arange(tok_local, dtype=jnp.int32)
    earlier = (token_pos[:, None] > token_pos[None, :]).astype(jnp.bfloat16)
    before = jnp.dot(earlier, live_hot, preferred_element_type=jnp.float32)
    rank = jnp.sum(before * live_hot.astype(jnp.float32), axis=1).astype(jnp.int32)
    counts = jnp.sum(owner_hot.astype(jnp.int32), axis=0)
    return dict(
        sens=sensitivity.reshape(tok_local, width), normed=normed, own_reward=own_reward,
        live=live, offset=offset, owner=owner, rank=rank, counts=counts,
        owner_hot=owner_hot, resp=token_pos // block_len, capacity=capacity,
        chosen_index=chosen_index, rejected_index=rejected_index, devices=devices,
        shard_rows=shard_rows, resp_local=resp_local, width=width, tok_local=tok_local,
    )


def lane_pad(a, lanes):
    return jnp.pad(a, ((0, 0), (0, lanes - a.shape[1])))[:, None, :]


def reward_grads(p, reward):
    responses = p["devices"] * p["resp_local"]
    all_resp = jnp.arange(responses, dtype=jnp.int32)
    sign_table = (p["chosen_index"][:, None] == all_resp[None, :]).astype(jnp.float32) - (
        p["rejected_index"][:, None] == all_resp[None, :]
    ).astype(jnp.float32)
    margin = jnp.sum(sign_table * reward[None, :], axis=1)
    push = -jax.nn.sigmoid(-margin)
    return jnp.sum(sign_table * push[:, None], axis=0)


def place_all(shard_rows, rows, targets, scale):
    scaled = (scale[:, None] * rows).astype(jnp.bfloat16)
    placing = (targets[None, :] == jnp.arange(shard_rows, dtype=jnp.int32)[:, None]).astype(
        jnp.bfloat16
    )
    return jnp.dot(placing, scaled, preferred_element_type=jnp.float32).astype(jnp.bfloat16)


def plain_finish(p, n_dev):
    devices, capacity, resp_local = p["devices"], p["capacity"], p["resp_local"]
    width = p["width"]
    cols = width // devices
    responses = devices * resp_local
    lanes = -(-max(cols, capacity, resp_local) // 128) * 128
    slot = jnp.where(p["live"], p["owner"] * capacity + p["rank"], -1)
    slot_match = slot[None, :] == jnp.arange(devices * capacity, dtype=jnp.int32)[:, None]
    outgoing = jnp.dot(
        slot_match.astype(jnp.bfloat16), p["sens"], preferred_element_type=jnp.float32
    ).astype(jnp.bfloat16)
    code = (p["offset"] + 1) * resp_local + p["resp"]
    codes = jnp.sum(jnp.where(slot_match, code[None, :], 0), axis=1)
    codes = codes.reshape(devices, capacity)
    target_out = codes // resp_local - 1
    resp_out = codes - codes // resp_local * resp_local
    normed_blocks = p["normed"].reshape(resp_local, devices, cols).transpose(1, 0, 2)
    meta = jnp.concatenate(
        [
            lane_pad(target_out.astype(jnp.float32), lanes),
            lane_pad(resp_out.astype(jnp.float32), lanes),
            lane_pad(jnp.broadcast_to(p["own_reward"][None, :], (devices, resp_local)), lanes),
            jnp.zeros((devices, 1, lanes), jnp.float32),
            jnp.pad(normed_blocks, ((0, 0), (0, 0), (0, lanes - cols))),
        ],
        axis=1,
    )
    extra = -meta.shape[1] % 8
    meta = jnp.pad(meta, ((0, 0), (0, extra), (0, 0)))
    meta_in, arrived = exchange(
        meta, outgoing.reshape(devices, capacity, width), devices, n_dev
    )
    targets = meta_in[:, 0, :capacity].astype(jnp.int32).reshape(devices * capacity)
    resp_in = meta_in[:, 1, :capacity].astype(jnp.int32)
    reward = meta_in[:, 2, :resp_local].reshape(responses)
    normed_in = meta_in[:, 4 : 4 + resp_local, :cols]
    reward_grad = reward_grads(p, reward).reshape(devices, resp_local)
    head_grad = jnp.sum(reward_grad[:, :, None] * normed_in, axis=(0, 1))
    resp_hot = resp_in[:, :, None] == jnp.arange(resp_local, dtype=jnp.int32)[None, None, :]
    scale = jnp.sum(jnp.where(resp_hot, reward_grad[:, None, :], 0.0), axis=2)
    total = devices * capacity
    owned = place_all(
        p["shard_rows"], arrived.reshape(total, width), targets, scale.reshape(total)
    )
    return owned, head_grad


def relay_local(*args):
    n_grp, n_dev = lax.axis_size("grp"), lax.axis_size("dev")
    shard_rows = VOCAB // args[-1].shape[0]
    rows_in, packed, where, slot_info, head, flag = relay_exchange(
        args, n_grp, n_dev, shard_rows // BLOCKS
    )

    def relayed(operands):
        rows, packed, where, slot_info, flag = operands

        def spread(o):
            return place_all(
                shard_rows, o[0], o[3][:, 0].reshape(-1).astype(jnp.int32),
                o[3][:, 1].reshape(-1),
            )

        return lax.cond(
            flag[1, 0] <= 0.0,
            lambda o: place_packed(shard_rows, o[2], o[1]),
            spread,
            (rows, packed, where, slot_info),
        )

    owned = lax.cond(
        flag[0, 0] <= 0.0,
        relayed,
        lambda operands: plain_finish(prepare(*args), n_dev)[0],
        (rows_in, packed, where, slot_info, flag),
    )
    return owned, head.reshape(-1)


def solution(mesh):
    placed = (
        P(("grp", "dev"), None),
        P(("grp", "dev"), None, None),
        P(("grp", "dev"), None),
        P(("grp", "dev")),
        P(),
        P(),
        P(),
        P(),
        P(),
    )
    return jax.shard_map(
        local,
        mesh=mesh,
        in_specs=placed,
        out_specs=(P(("grp", "dev"), None), P(("grp", "dev"))),
        check_vma=False,
    )
```

```python
import functools

import jax
import jax.numpy as jnp
from jax import lax
from jax.experimental import pallas as pl
from jax.experimental.pallas import tpu as pltpu
from jax.sharding import PartitionSpec as P

VOCAB = 128256
MESH = pl.DeviceIdType.MESH


def exchange_kernel(n, n_dev, meta_ref, rows_ref, meta_out, rows_out, send_sem, recv_sem, own_sem):
    me = lax.axis_index("grp") * n_dev + lax.axis_index("dev")

    def coord(t):
        return (t // n_dev, lax.rem(t, n_dev))

    barrier = pltpu.get_barrier_semaphore()

    def greet(k, c):
        t = lax.rem(me + k, n)
        pl.semaphore_signal(barrier, inc=1, device_id=coord(t), device_id_type=MESH)
        return c

    lax.fori_loop(1, n, greet, 0)
    own = [
        pltpu.make_async_copy(src.at[me], dst.at[me], own_sem.at[i])
        for i, (src, dst) in enumerate(((meta_ref, meta_out), (rows_ref, rows_out)))
    ]
    for c in own:
        c.start()
    pl.semaphore_wait(barrier, n - 1)

    def copies(src_block, dst_block, to):
        return [
            pltpu.make_async_remote_copy(
                src_ref=src.at[src_block],
                dst_ref=dst.at[dst_block],
                send_sem=send_sem.at[i, src_block],
                recv_sem=recv_sem.at[i, dst_block],
                device_id=coord(to),
                device_id_type=MESH,
            )
            for i, (src, dst) in enumerate(((meta_ref, meta_out), (rows_ref, rows_out)))
        ]

    def send(k, c):
        t = lax.rem(me + k, n)
        for cp in copies(t, me, t):
            cp.start()
        return c

    lax.fori_loop(1, n, send, 0)

    def finish(k, c):
        t = lax.rem(me + k, n)
        for cp in copies(t, me, t):
            cp.wait_send()
        s = lax.rem(me + n - k, n)
        for cp in copies(s, s, s):
            cp.wait_recv()
        return c

    lax.fori_loop(1, n, finish, 0)
    for c in own:
        c.wait()


def exchange(meta, rows, n, n_dev):
    anyspec = pl.BlockSpec(memory_space=pl.ANY)
    return pl.pallas_call(
        functools.partial(exchange_kernel, n, n_dev),
        out_shape=(
            jax.ShapeDtypeStruct(meta.shape, meta.dtype),
            jax.ShapeDtypeStruct(rows.shape, rows.dtype),
        ),
        in_specs=[anyspec, anyspec],
        out_specs=(anyspec, anyspec),
        scratch_shapes=[
            pltpu.SemaphoreType.DMA((2, n)),
            pltpu.SemaphoreType.DMA((2, n)),
            pltpu.SemaphoreType.DMA((2,)),
        ],
        compiler_params=pltpu.CompilerParams(collective_id=1, has_side_effects=True),
    )(meta, rows)


GROUP = 8
NEAR = 32
FAR = 16
FWD = 8
AHEAD = 4
WINDOW = 256
BLOCKS = 3
CHUNK = 512
EARLY = 8
LATE = 12


def near_row(k):
    return k * NEAR + (k // EARLY) * 128 + (k // LATE) * 128


def far_row(k):
    return 256 + k * FAR + (k // EARLY) * 128


def log2(x):
    return x.bit_length() - 1


def relay_kernel(n_grp, n_dev, block_rows, ids_ref, sens_ref, hidden_ref, length_ref, gain_ref,
                 weight_ref, chosen_ref, rejected_ref, owner_ref,
                 rows_out, packed, where_out, slot_out, head_out, flag_out,
                 sens_v, select, slots_v, pout, fm_out, pmeta_out,
                 rin, fin, fm_in, pin, pmeta_in, fwd, fwd_meta, fmeta_in, picks, scales,
                 sens_sems, fm_sems, near_sems, far_sems, piece_sems, pm_sems, fwd_sems,
                 fwdm_sems, save_sems):
    g = lax.axis_index("grp")
    v = lax.axis_index("dev")
    hd = n_dev // 2
    local_n = n_grp * hd
    half = v // hd
    u = lax.rem(v, hd)
    me = g * n_dev + v
    n = n_grp * n_dev
    pieces = n_grp + 1
    direct = local_n * (NEAR + FAR)
    far_base = local_n * NEAR
    other = 1 - half
    width = sens_ref.shape[1]
    f32 = jnp.float32
    chunks = width // CHUNK
    count = pieces * GROUP
    shard_rows = block_rows * BLOCKS
    i32 = jnp.int32
    rows_rows = (((1,), (1,)), ((), ()))

    def iota(rows, cols, axis):
        return lax.broadcasted_iota(i32, (rows, cols), axis)

    def coord(t):
        return (t // n_dev, lax.rem(t, n_dev))

    barrier = pltpu.get_barrier_semaphore()

    def greet(k, c):
        pl.semaphore_signal(
            barrier, inc=1, device_id=coord(lax.rem(me + k, n)), device_id_type=MESH
        )
        return c

    lax.fori_loop(1, n, greet, 0)
    def fetch(c):
        return pltpu.make_async_copy(
            sens_ref.at[:, pl.ds(c * CHUNK, CHUNK)], sens_v.at[c], sens_sems.at[c]
        )

    for c in range(chunks):
        fetch(c).start()

    eye0, eye1 = iota(128, 128, 0), iota(128, 128, 1)
    tri = jnp.where(eye0 < eye1, 1.0, 0.0)
    resp_local, block_len = ids_ref.shape
    resp_row, resp_pos = iota(resp_local, block_len, 0), iota(resp_local, block_len, 1)
    ids = ids_ref[...]
    length = jnp.zeros((resp_local, block_len), i32)
    for r in range(resp_local):
        length = jnp.where(resp_row == r, length_ref[r], length)
    live_all = resp_pos < length
    shard = jnp.floor((ids.astype(f32) + 0.5) * (1.0 / shard_rows)).astype(i32)
    above = ids - shard * shard_rows + 1
    owner_all = jnp.zeros((resp_local, block_len), i32)
    for k in range(n):
        owner_all = jnp.where(shard == k, owner_ref[k], owner_all)
    owner_g = owner_all >> log2(n_dev)
    owner_v = owner_all & (n_dev - 1)
    owner_u = owner_v & (hd - 1)
    near_all = (owner_v >> log2(hd)) == half
    away_all = (((owner_g - g) & (n_grp - 1)) << log2(hd)) + ((owner_u - u) & (hd - 1))
    dev_row = iota(n, 128, 0)
    filled_to = jnp.zeros((n, 1), f32)
    hots, ranks = [], []
    for r in range(resp_local):
        live = live_all[r : r + 1]
        hot = jnp.where((dev_row == owner_all[r : r + 1]) & live, 1.0, 0.0)
        ahead = jnp.dot(hot, tri, preferred_element_type=f32) + filled_to
        ranks.append(jnp.sum(hot * ahead, axis=0, keepdims=True))
        filled_to = filled_to + jnp.sum(hot, axis=1, keepdims=True)
        hots.append(hot)
    dev_far = ((dev_row & (n_dev - 1)) >> log2(hd)) != half
    over_out = jnp.where(dev_far, jnp.maximum(filled_to - FAR, 0.0), 0.0)
    lower = jnp.where(iota(n, n, 0) > iota(n, n, 1), 1.0, 0.0)
    base_out = jnp.dot(lower, over_out, preferred_element_type=f32)
    over_row = jnp.sum(
        jnp.where(dev_row == iota(n, 128, 1), over_out, 0.0), axis=0, keepdims=True
    )
    code_hi = jnp.zeros((n, 128), f32)
    code_lo = jnp.zeros((n, 128), f32)
    code_resp = jnp.zeros((n, 128), f32)
    piece_meta = jnp.zeros((count, 128), f32)
    for r in range(resp_local):
        live, near = live_all[r : r + 1], near_all[r : r + 1]
        away, rank = away_all[r : r + 1], ranks[r]
        place_j = jnp.sum(hots[r] * base_out, axis=0, keepdims=True) + rank - FAR
        level = jnp.floor((place_j + 0.5) * (1.0 / pieces))
        piece = direct + (place_j - pieces * level) * GROUP + level
        piece = jnp.where(place_j < count, piece, -1.0).astype(i32)
        rank = rank.astype(i32)
        slot = jnp.where(
            near,
            away * NEAR + rank,
            jnp.where(rank < FAR, far_base + away * FAR + rank, piece),
        )
        slot = jnp.where(live, slot, -1)
        select[:, pl.ds(r * 128, 128)] = jnp.where(
            iota(direct + 48, 128, 0) == slot, 1.0, 0.0
        ).astype(jnp.bfloat16)
        lane_at = jnp.where(near, (away & 3) * NEAR, (away & 7) * FAR) + rank
        shown = live & (near | (rank < FAR))
        at_hot = jnp.where(eye0 == jnp.where(shown, lane_at, -1), 1.0, 0.0)
        hi = (above[r : r + 1] >> 6).astype(f32)
        lo = (above[r : r + 1] & 63).astype(f32)
        resp = (iota(1, 128, 1) * 0 + (me * resp_local + r)).astype(f32)
        code_hi += lax.dot_general(hots[r] * hi, at_hot, rows_rows, preferred_element_type=f32)
        code_lo += lax.dot_general(hots[r] * lo, at_hot, rows_rows, preferred_element_type=f32)
        code_resp += lax.dot_general(
            hots[r] * resp, at_hot, rows_rows, preferred_element_type=f32
        )
        feature = jnp.where(eye0 == 0, 1.0, 0.0)
        for i, row in (
            (1, owner_g[r : r + 1].astype(f32)), (2, owner_u[r : r + 1].astype(f32)),
            (3, resp), (4, hi), (5, lo),
        ):
            feature = jnp.where(eye0 == i, row, feature)
        in_piece = jnp.where(iota(count, 128, 0) + direct == slot, 1.0, 0.0)
        piece_meta += lax.dot_general(
            in_piece, feature, rows_rows, preferred_element_type=f32
        )
    pmeta_out[...] = piece_meta.reshape(pieces, GROUP, 128)

    hidden = hidden_ref[...].astype(f32)
    square = jnp.sum(hidden * hidden, axis=1, keepdims=True) * (1.0 / width)
    normed = hidden / jnp.sqrt(square + 1e-05) * gain_ref[...]
    own_reward = jnp.sum(normed * weight_ref[...], axis=1, keepdims=True)
    reward_row = jnp.sum(
        jnp.where(resp_pos == me * resp_local + resp_row, own_reward, 0.0),
        axis=0, keepdims=True,
    )
    fm_out[:, 0, :] = jnp.broadcast_to(reward_row, (n, 128))
    fm_out[:, 1, :] = (code_hi * 64.0 + code_lo) * 128.0 + code_resp
    fm_out[:, 2, :] = jnp.broadcast_to(over_row, (n, 128))
    fm_out[:, 3, :] = jnp.zeros((n, 128), f32)
    for d in range(n):
        fm_out[d, 4:8, :] = normed[:, d * 128 : (d + 1) * 128]
    fm_in[0] = fm_out[me]

    def build_far(c, carry):
        cols = pl.ds(pl.multiple_of(c * CHUNK, CHUNK), CHUNK)
        fetch(c).wait()
        got = jnp.dot(select[pl.ds(far_base, direct + 48 - far_base), :], sens_v[c],
                      preferred_element_type=f32)
        slots_v[pl.ds(far_base, direct - far_base), cols] = got[
            : direct - far_base
        ].astype(jnp.bfloat16)
        pout[:, :, cols] = got[direct - far_base : direct - far_base + count].reshape(
            pieces, GROUP, CHUNK
        ).astype(jnp.bfloat16)
        return carry

    lax.fori_loop(0, chunks, build_far, 0)
    pl.semaphore_wait(barrier, n - 1)

    def remote(src, dst, send_sem, recv_sem, to):
        return pltpu.make_async_remote_copy(
            src_ref=src, dst_ref=dst, send_sem=send_sem, recv_sem=recv_sem,
            device_id=to, device_id_type=MESH,
        )

    def partner(k, side):
        return lax.rem(g + k // hd, n_grp), side * hd + lax.rem(u + lax.rem(k, hd), hd)

    def piece_target(q):
        if q < n_grp:
            return (lax.rem(g + q, n_grp), other * hd + u)
        return (g, other * hd + lax.rem(u + hd // 2, hd))

    piece_copies = []
    for q in range(pieces):
        to = piece_target(q)
        piece_copies.append(
            remote(pout.at[q], pin.at[q],
                   piece_sems.at[0, q], piece_sems.at[1, q], to)
        )
        piece_copies.append(
            remote(pmeta_out.at[q], pmeta_in.at[q], pm_sems.at[0, q], pm_sems.at[1, q], to)
        )
    for cp in piece_copies:
        cp.start()

    def fm_copy(r):
        side = lax.rem(half + r // local_n, 2)
        tg, tv = partner(lax.rem(r, local_n), side)
        return remote(fm_out.at[tg * n_dev + tv], fm_in.at[r], fm_sems.at[0, r],
                      fm_sems.at[1, r], (tg, tv))

    def near_copy(k):
        return remote(
            slots_v.at[pl.ds(k * NEAR, NEAR)], rin.at[pl.ds(near_row(k), NEAR)],
            near_sems.at[0, k], near_sems.at[1, k], partner(k, half),
        )

    def far_copy(k):
        return remote(
            slots_v.at[pl.ds(far_base + k * FAR, FAR)], rin.at[pl.ds(far_row(k), FAR)],
            far_sems.at[0, k], far_sems.at[1, k], partner(k, other),
        )

    def fwd_copies(k):
        to = partner(k, half)
        return [
            remote(fwd.at[k], fin.at[pl.ds(k * FWD, FWD)], fwd_sems.at[0, k], fwd_sems.at[1, k], to),
            remote(fwd_meta.at[k], fmeta_in.at[k], fwdm_sems.at[0, k], fwdm_sems.at[1, k], to),
        ]

    def send_fm(r, c):
        fm_copy(r).start()
        return c

    lax.fori_loop(1, n, send_fm, 0)

    def send_far(k, c):
        far_copy(k).start()
        return c

    def send_both(k, c):
        far_copy(k).start()
        near_copy(k).start()
        return c

    def send_near(k, c):
        near_copy(k).start()
        return c

    lax.fori_loop(0, AHEAD, send_far, 0)

    def build_near(c, carry):
        cols = pl.ds(pl.multiple_of(c * CHUNK, CHUNK), CHUNK)
        got = jnp.dot(select[pl.ds(0, far_base), :], sens_v[c],
                      preferred_element_type=f32).astype(jnp.bfloat16)
        slots_v[pl.ds(0, far_base), cols] = got
        rin[pl.ds(0, NEAR), cols] = got[:NEAR]
        return carry

    lax.fori_loop(0, chunks, build_near, 0)
    lax.fori_loop(1, AHEAD, send_near, 0)
    lax.fori_loop(AHEAD, local_n, send_both, 0)

    for cp in piece_copies:
        cp.wait_recv()
    marks = pmeta_in[...].reshape(count, 128)
    used = marks[:, 0:1] > 0.0
    dst_g = marks[:, 1:2].astype(jnp.int32)
    dst_u = marks[:, 2:3].astype(jnp.int32)
    dst = ((dst_g - g) & (n_grp - 1)) * hd + ((dst_u - u) & (hd - 1))
    lane = lax.broadcasted_iota(jnp.int32, (count, 128), 1)
    hot = jnp.where((lane == dst) & used, 1.0, 0.0)
    row_i = lax.broadcasted_iota(jnp.int32, (count, count), 0)
    col_i = lax.broadcasted_iota(jnp.int32, (count, count), 1)
    earlier = jnp.where(row_i > col_i, 1.0, 0.0)
    before = jnp.dot(earlier, hot, preferred_element_type=f32)
    rank = jnp.sum(before * hot, axis=1, keepdims=True).astype(jnp.int32)
    slot = jnp.where(used & (rank < FWD), dst * FWD + rank, -1)
    place = jnp.where(lane == slot, 1.0, 0.0)
    contract = (((0,), (0,)), ((), ()))

    def gather(c, carry):
        cols = pl.ds(pl.multiple_of(c * CHUNK, CHUNK), CHUNK)
        rows = pin[:, :, cols].astype(f32).reshape(count, CHUNK)
        out = lax.dot_general(place, rows, contract, preferred_element_type=f32)
        out = out.reshape(local_n, FWD, CHUNK).astype(jnp.bfloat16)
        fwd[:, :, cols] = out
        fin[pl.ds(0, FWD), cols] = out[0]
        return carry

    lax.fori_loop(0, width // CHUNK, gather, 0)
    out_meta = lax.dot_general(place, marks, contract, preferred_element_type=f32)
    out_meta = out_meta.reshape(local_n, FWD, 128)
    fwd_meta[...] = out_meta
    fmeta_in[0] = out_meta[0]

    def send_fwd(k, c):
        for cp in fwd_copies(k):
            cp.start()
        return c

    lax.fori_loop(1, local_n, send_fwd, 0)

    def wait_fm(r, c):
        cp = fm_copy(r)
        cp.wait_send()
        cp.wait_recv()
        return c

    lax.fori_loop(1, n, wait_fm, 0)

    def source(r):
        a, b = (r & (local_n - 1)) // hd, r & (hd - 1)
        side = (half - r // local_n) & 1
        sg, su = (g - a) & (n_grp - 1), (u - b) & (hd - 1)
        return sg, su, sg * n_dev + side * hd + su

    reward = jnp.sum(fm_in[:, 0, :], axis=0, keepdims=True)
    pairs = chosen_ref.shape[0]
    pair_row = iota(pairs, 1, 0)
    chosen = jnp.zeros((pairs, 1), i32)
    rejected = jnp.zeros((pairs, 1), i32)
    for k in range(pairs):
        chosen = jnp.where(pair_row == k, chosen_ref[k], chosen)
        rejected = jnp.where(pair_row == k, rejected_ref[k], rejected)
    pair_lane = iota(pairs, 128, 1)
    sign = jnp.where(chosen == pair_lane, 1.0, 0.0) - jnp.where(
        rejected == pair_lane, 1.0, 0.0
    )
    margin = jnp.sum(sign * reward, axis=1, keepdims=True)
    push = -1.0 / (1.0 + jnp.exp(margin))
    reward_grad = jnp.sum(sign * push, axis=0, keepdims=True)
    grad_col = jnp.sum(jnp.where(eye0 == eye1, reward_grad, 0.0), axis=1, keepdims=True)
    src_lane = lax.broadcasted_iota(jnp.int32, (n, 128), 1)
    _, _, src = source(lax.broadcasted_iota(jnp.int32, (n, 128), 0))
    head = jnp.zeros((1, 128), f32)
    for j in range(4):
        part = jnp.where(src_lane == src * 4 + j, reward_grad, 0.0)
        coef = jnp.sum(part, axis=1, keepdims=True)
        head = head + jnp.sum(coef * fm_in[:, 4 + j, :], axis=0, keepdims=True)
    head_out[...] = head

    over = fm_in[:, 2, :]
    over_base = jnp.dot(over, tri, preferred_element_type=f32)
    here = lax.broadcasted_iota(jnp.int32, (local_n, n), 0)
    from_g, from_u, _ = source(lax.broadcasted_iota(jnp.int32, (local_n, n), 1))
    load = jnp.zeros((local_n, 128), f32)
    for q in range(pieces):
        part = jnp.floor((over_base + over - q + pieces - 0.5) * (1.0 / pieces)) - jnp.floor(
            (over_base - q + pieces - 0.5) * (1.0 / pieces)
        )
        if q < n_grp:
            at = ((from_g + q) & (n_grp - 1)) * hd + from_u
        else:
            at = from_g * hd + ((from_u + hd // 2) & (hd - 1))
        lands = jnp.where(at == here, 1.0, 0.0)
        load = load + jnp.dot(lands, part, preferred_element_type=f32)
    excess = jnp.maximum(
        jnp.max(jnp.max(load, axis=1, keepdims=True), axis=0, keepdims=True) - FWD,
        jnp.max(jnp.sum(over, axis=1, keepdims=True), axis=0, keepdims=True) - count,
    )

    def code_row(start, size):
        return jnp.sum(fm_in[pl.ds(start, size), 1, :], axis=0, keepdims=True)

    code_rows = [
        code_row(0, 4), code_row(4, 4), code_row(local_n, 8),
        code_row(8, 4), code_row(local_n + 8, 8), code_row(12, 4),
    ]
    sub = lax.broadcasted_iota(jnp.int32, (8, 128), 0)
    resp_id = eye0
    total = packed.shape[0]
    packed_id = lax.broadcasted_iota(jnp.int32, (total, 128), 0)

    def index_tile(i, target, resp, filled, worst, found):
        begin = sub * block_rows
        inside = (target >= begin) & (target < begin + block_rows) & (target >= 0)
        hot_b = jnp.where(inside, 1.0, 0.0)
        ahead = jnp.dot(hot_b, tri, preferred_element_type=f32) + filled
        rank_b = jnp.sum(hot_b * ahead, axis=0, keepdims=True).astype(jnp.int32)
        block = jnp.sum(jnp.where(inside, sub, 0), axis=0, keepdims=True)
        live = target >= 0
        ok = live & (rank_b < WINDOW)
        pos = jnp.where(ok, block * WINDOW + rank_b, -1)
        pick = jnp.where(packed_id == pos, 1.0, 0.0)
        picks[i // 2, :, pl.ds(i % 2 * 128, 128)] = pick.astype(jnp.bfloat16)
        scale = jnp.sum(jnp.where(resp_id == resp, grad_col, 0.0), axis=0, keepdims=True)
        scale = jnp.where(live, scale, 0.0)
        got = jnp.sum(pick * scale, axis=1, keepdims=True)
        marked = jnp.where(live, target + 1, 0)
        digits = jnp.where(sub == 0, marked >> 6, jnp.where(sub == 1, marked & 63, 0))
        found = found + lax.dot_general(
            digits.astype(f32), pick, rows_rows, preferred_element_type=f32
        )
        slot_out[i, 0:1, :] = (marked - 1).astype(f32)
        slot_out[i, 1:2, :] = scale
        filled = filled + jnp.sum(hot_b, axis=1, keepdims=True)
        worst = jnp.maximum(worst, jnp.max(filled, axis=0, keepdims=True))
        return filled, worst, found, got

    slot_out[...] = jnp.zeros_like(slot_out)
    filled = jnp.zeros((8, 1), f32)
    worst = jnp.zeros((1, 1), f32)
    found = jnp.zeros((8, total), f32)
    for i, row in enumerate(code_rows):
        code = row.astype(jnp.int32)
        filled, worst, found, got = index_tile(
            i, (code >> 7) - 1, code & 127, filled, worst, found
        )
        if i % 2 == 0:
            scales[i // 2] = got
        else:
            scales[i // 2] = scales[i // 2] + got

    def pack(seg, first):
        def col(c, carry):
            cols = pl.ds(pl.multiple_of(c * CHUNK, CHUNK), CHUNK)
            got = jnp.dot(picks[seg], rin[pl.ds(seg * 256, 256), cols],
                          preferred_element_type=f32)
            got = (scales[seg] * got).astype(jnp.bfloat16)
            packed[:, cols] = got if first else packed[:, cols] + got
            return carry

        lax.fori_loop(0, width // CHUNK, col, 0)

    def save(i, src, start, size):
        return pltpu.make_async_copy(src, rows_out.at[pl.ds(start, size)], save_sems.at[i])

    def wait_far(k, c):
        cp = far_copy(k)
        cp.wait_send()
        cp.wait_recv()
        return c

    def wait_near(k, c):
        cp = near_copy(k)
        cp.wait_send()
        cp.wait_recv()
        return c

    saves = [save(i, rin.at[pl.ds(i * 256, 256)], i * 256, 256) for i in range(3)]
    lax.fori_loop(1, EARLY, wait_near, 0)
    saves[0].start()
    pack(0, True)
    lax.fori_loop(0, EARLY, wait_far, 0)
    lax.fori_loop(EARLY, LATE, wait_near, 0)
    saves[1].start()
    pack(1, False)
    for cp in piece_copies:
        cp.wait_send()
    lax.fori_loop(EARLY, local_n, wait_far, 0)
    lax.fori_loop(LATE, local_n, wait_near, 0)
    saves[2].start()
    pack(2, False)

    def wait_fwd(k, c):
        for cp in fwd_copies(k):
            cp.wait_send()
            cp.wait_recv()
        return c

    lax.fori_loop(1, local_n, wait_fwd, 0)
    fmeta = fmeta_in[...].reshape(128, 128)
    pick_rows = jnp.where(
        lax.broadcasted_iota(jnp.int32, (8, 128), 0)
        == lax.broadcasted_iota(jnp.int32, (8, 128), 1), 1.0, 0.0
    )
    meta_rows = lax.dot_general(pick_rows, fmeta, rows_rows, preferred_element_type=f32)
    meta_rows = meta_rows.astype(jnp.int32)
    target = meta_rows[4:5] * 64 + meta_rows[5:6] - 1
    filled, worst, found, got = index_tile(6, target, meta_rows[3:4], filled, worst, found)
    scales[3] = got

    for c in range(width // CHUNK):
        cols = pl.ds(c * CHUNK, CHUNK)
        got = jnp.dot(picks[3, :, pl.ds(0, 128)], fin[:, cols], preferred_element_type=f32)
        packed[:, cols] = packed[:, cols] + (scales[3] * got).astype(jnp.bfloat16)
    saves.append(save(3, fin, direct, local_n * FWD))
    saves[3].start()
    where_out[...] = found[0:1] * 64.0 + found[1:2] - 1.0 + jnp.zeros((8, total), f32)
    flag_out[...] = jnp.where(excess > 0.0, 2, jnp.where(worst > WINDOW, 1, 0))
    for cp in saves:
        cp.wait()


def relay_exchange(args, n_grp, n_dev, block_rows):
    ids, sens, hidden, lengths, gain, weight, chosen, rejected, owner = args
    resp_local, block_len, width = sens.shape
    n = n_grp * n_dev
    local_n = n // 2
    pieces = n_grp + 1
    direct = local_n * (NEAR + FAR)
    rows = direct + local_n * FWD
    total = BLOCKS * WINDOW
    anyspec = pl.BlockSpec(memory_space=pl.ANY)
    vmem = pl.BlockSpec(memory_space=pltpu.VMEM)
    smem = pl.BlockSpec(memory_space=pltpu.SMEM)
    sem = pltpu.SemaphoreType.DMA
    bf16, f32 = jnp.bfloat16, jnp.float32
    return pl.pallas_call(
        functools.partial(relay_kernel, n_grp, n_dev, block_rows),
        out_shape=(
            jax.ShapeDtypeStruct((rows, width), bf16),
            jax.ShapeDtypeStruct((total, width), bf16),
            jax.ShapeDtypeStruct((8, total), f32),
            jax.ShapeDtypeStruct((rows // 128, 8, 128), f32),
            jax.ShapeDtypeStruct((1, 128), f32),
            jax.ShapeDtypeStruct((1, 1), jnp.int32),
        ),
        in_specs=[vmem, anyspec, vmem, smem, vmem, vmem, smem, smem, smem],
        out_specs=(anyspec, vmem, vmem, vmem, vmem, vmem),
        scratch_shapes=[
            pltpu.VMEM((width // CHUNK, resp_local * block_len, CHUNK), bf16),
            pltpu.VMEM((direct + 48, resp_local * block_len), bf16),
            pltpu.VMEM((direct, width), bf16),
            pltpu.VMEM((pieces, GROUP, width), bf16),
            pltpu.VMEM((n, 8, 128), f32),
            pltpu.VMEM((pieces, GROUP, 128), f32),
            pltpu.VMEM((direct, width), bf16),
            pltpu.VMEM((local_n * FWD, width), bf16),
            pltpu.VMEM((n, 8, 128), f32),
            pltpu.VMEM((pieces, GROUP, width), bf16),
            pltpu.VMEM((pieces, GROUP, 128), f32),
            pltpu.VMEM((local_n, FWD, width), bf16),
            pltpu.VMEM((local_n, FWD, 128), f32),
            pltpu.VMEM((local_n, FWD, 128), f32),
            pltpu.VMEM((4, total, 256), bf16),
            pltpu.VMEM((4, total, 1), f32),
            sem((width // CHUNK,)),
            sem((2, n)),
            sem((2, local_n)),
            sem((2, local_n)),
            sem((2, pieces)),
            sem((2, pieces)),
            sem((2, local_n)),
            sem((2, local_n)),
            sem((4,)),
        ],
        compiler_params=pltpu.CompilerParams(
            collective_id=0, has_side_effects=True, vmem_limit_bytes=46 * 1024 * 1024
        ),
    )(ids, sens.reshape(-1, width), hidden, lengths, gain[None, :], weight[None, :], chosen,
      rejected, owner)


def place_kernel(where_ref, packed_ref, out_ref, onehot, outbuf, out_sems):
    total, width = packed_ref.shape
    shard_rows = out_ref.shape[0]
    block_rows = shard_rows // BLOCKS
    padded = -(-block_rows // 16) * 16
    chunks = width // CHUNK
    slots = outbuf.shape[0]

    def put(b, c, slot):
        return pltpu.make_async_copy(
            outbuf.at[slot, pl.ds(0, block_rows)],
            out_ref.at[pl.ds(b * block_rows, block_rows), pl.ds(c * CHUNK, CHUNK)],
            out_sems.at[slot],
        )

    for b in range(BLOCKS):
        row_id = lax.broadcasted_iota(jnp.int32, (padded, WINDOW), 0) + b * block_rows
        target = where_ref[0:1, pl.ds(b * WINDOW, WINDOW)].astype(jnp.int32)
        onehot[...] = jnp.where(row_id == target, 1.0, 0.0).astype(jnp.bfloat16)
        for c in range(chunks):
            step = b * chunks + c
            if step >= slots:
                put((step - slots) // chunks, (step - slots) % chunks, step % slots).wait()
            outbuf[step % slots] = jnp.dot(
                onehot[...], packed_ref[pl.ds(b * WINDOW, WINDOW), pl.ds(c * CHUNK, CHUNK)],
                preferred_element_type=jnp.float32,
            ).astype(jnp.bfloat16)
            put(b, c, step % slots).start()
    steps = BLOCKS * chunks
    for step in range(steps - slots, steps):
        put(step // chunks, step % chunks, step % slots).wait()


def place_packed(shard_rows, where, packed):
    total, width = packed.shape
    chunks = width // CHUNK
    padded = -(-(shard_rows // BLOCKS) // 16) * 16
    vmem = pl.BlockSpec(memory_space=pltpu.VMEM)
    anyspec = pl.BlockSpec(memory_space=pl.ANY)
    return pl.pallas_call(
        place_kernel,
        out_shape=jax.ShapeDtypeStruct((shard_rows, width), packed.dtype),
        in_specs=[vmem, vmem],
        out_specs=anyspec,
        scratch_shapes=[
            pltpu.VMEM((padded, WINDOW), jnp.bfloat16),
            pltpu.VMEM((4, padded, CHUNK), jnp.bfloat16),
            pltpu.SemaphoreType.DMA((4,)),
        ],
        compiler_params=pltpu.CompilerParams(vmem_limit_bytes=40 * 1024 * 1024),
    )(where, packed)


def local(token_ids, sensitivity, last_hidden, lengths, norm_gain, reward_head,
          chosen_index, rejected_index, shard_owner):
    args = (token_ids, sensitivity, last_hidden, lengths, norm_gain, reward_head,
            chosen_index, rejected_index, shard_owner)
    resp_local, block_len = token_ids.shape
    devices = shard_owner.shape[0]
    n_grp, n_dev = lax.axis_size("grp"), lax.axis_size("dev")
    capacity = max(2, (2 * resp_local * block_len + devices - 1) // devices)
    shard_rows, width = VOCAB // devices, sensitivity.shape[2]
    if (capacity == NEAR and devices == 32 and n_grp in (1, 2, 4, 8) and n_dev % 4 == 0
            and resp_local == 4 and shard_rows % (8 * BLOCKS) == 0 and shard_rows < 64 * 250
            and width % CHUNK == 0 and width // devices == 128 and block_len == 128):
        return relay_local(*args)
    prep = prepare(*args)
    return plain_finish(prep, n_dev)


def prepare(token_ids, sensitivity, last_hidden, lengths, norm_gain, reward_head,
            chosen_index, rejected_index, shard_owner):
    resp_local, block_len = token_ids.shape
    width = sensitivity.shape[2]
    tok_local = resp_local * block_len
    devices = shard_owner.shape[0]
    shard_rows = VOCAB // devices
    capacity = max(2, (2 * tok_local + devices - 1) // devices)
    hidden = last_hidden.astype(jnp.float32)
    normed = (
        hidden / jnp.sqrt(jnp.mean(hidden * hidden, axis=-1, keepdims=True) + 1e-05) * norm_gain
    )
    own_reward = jnp.sum(normed * reward_head, axis=-1)

    positions = jnp.arange(block_len, dtype=jnp.int32)
    live = (positions[None, :] < lengths[:, None]).reshape(tok_local)
    ids = token_ids.reshape(tok_local)
    shard_of = ids // shard_rows
    offset = ids - shard_of * shard_rows
    shard_hot = shard_of[:, None] == jnp.arange(devices, dtype=jnp.int32)[None, :]
    owner = jnp.sum(jnp.where(shard_hot, shard_owner[None, :], 0), axis=1)
    owner_hot = (owner[:, None] == jnp.arange(devices, dtype=jnp.int32)[None, :]) & live[:, None]
    live_hot = owner_hot.astype(jnp.bfloat16)
    token_pos = jnp.arange(tok_local, dtype=jnp.int32)
    earlier = (token_pos[:, None] > token_pos[None, :]).astype(jnp.bfloat16)
    before = jnp.dot(earlier, live_hot, preferred_element_type=jnp.float32)
    rank = jnp.sum(before * live_hot.astype(jnp.float32), axis=1).astype(jnp.int32)
    counts = jnp.sum(owner_hot.astype(jnp.int32), axis=0)
    return dict(
        sens=sensitivity.reshape(tok_local, width), normed=normed, own_reward=own_reward,
        live=live, offset=offset, owner=owner, rank=rank, counts=counts,
        owner_hot=owner_hot, resp=token_pos // block_len, capacity=capacity,
        chosen_index=chosen_index, rejected_index=rejected_index, devices=devices,
        shard_rows=shard_rows, resp_local=resp_local, width=width, tok_local=tok_local,
    )


def lane_pad(a, lanes):
    return jnp.pad(a, ((0, 0), (0, lanes - a.shape[1])))[:, None, :]


def reward_grads(p, reward):
    responses = p["devices"] * p["resp_local"]
    all_resp = jnp.arange(responses, dtype=jnp.int32)
    sign_table = (p["chosen_index"][:, None] == all_resp[None, :]).astype(jnp.float32) - (
        p["rejected_index"][:, None] == all_resp[None, :]
    ).astype(jnp.float32)
    margin = jnp.sum(sign_table * reward[None, :], axis=1)
    push = -jax.nn.sigmoid(-margin)
    return jnp.sum(sign_table * push[:, None], axis=0)


def place_all(shard_rows, rows, targets, scale):
    scaled = (scale[:, None] * rows).astype(jnp.bfloat16)
    placing = (targets[None, :] == jnp.arange(shard_rows, dtype=jnp.int32)[:, None]).astype(
        jnp.bfloat16
    )
    return jnp.dot(placing, scaled, preferred_element_type=jnp.float32).astype(jnp.bfloat16)


def plain_finish(p, n_dev):
    devices, capacity, resp_local = p["devices"], p["capacity"], p["resp_local"]
    width = p["width"]
    cols = width // devices
    responses = devices * resp_local
    lanes = -(-max(cols, capacity, resp_local) // 128) * 128
    slot = jnp.where(p["live"], p["owner"] * capacity + p["rank"], -1)
    slot_match = slot[None, :] == jnp.arange(devices * capacity, dtype=jnp.int32)[:, None]
    outgoing = jnp.dot(
        slot_match.astype(jnp.bfloat16), p["sens"], preferred_element_type=jnp.float32
    ).astype(jnp.bfloat16)
    code = (p["offset"] + 1) * resp_local + p["resp"]
    codes = jnp.sum(jnp.where(slot_match, code[None, :], 0), axis=1)
    codes = codes.reshape(devices, capacity)
    target_out = codes // resp_local - 1
    resp_out = codes - codes // resp_local * resp_local
    normed_blocks = p["normed"].reshape(resp_local, devices, cols).transpose(1, 0, 2)
    meta = jnp.concatenate(
        [
            lane_pad(target_out.astype(jnp.float32), lanes),
            lane_pad(resp_out.astype(jnp.float32), lanes),
            lane_pad(jnp.broadcast_to(p["own_reward"][None, :], (devices, resp_local)), lanes),
            jnp.zeros((devices, 1, lanes), jnp.float32),
            jnp.pad(normed_blocks, ((0, 0), (0, 0), (0, lanes - cols))),
        ],
        axis=1,
    )
    extra = -meta.shape[1] % 8
    meta = jnp.pad(meta, ((0, 0), (0, extra), (0, 0)))
    meta_in, arrived = exchange(
        meta, outgoing.reshape(devices, capacity, width), devices, n_dev
    )
    targets = meta_in[:, 0, :capacity].astype(jnp.int32).reshape(devices * capacity)
    resp_in = meta_in[:, 1, :capacity].astype(jnp.int32)
    reward = meta_in[:, 2, :resp_local].reshape(responses)
    normed_in = meta_in[:, 4 : 4 + resp_local, :cols]
    reward_grad = reward_grads(p, reward).reshape(devices, resp_local)
    head_grad = jnp.sum(reward_grad[:, :, None] * normed_in, axis=(0, 1))
    resp_hot = resp_in[:, :, None] == jnp.arange(resp_local, dtype=jnp.int32)[None, None, :]
    scale = jnp.sum(jnp.where(resp_hot, reward_grad[:, None, :], 0.0), axis=2)
    total = devices * capacity
    owned = place_all(
        p["shard_rows"], arrived.reshape(total, width), targets, scale.reshape(total)
    )
    return owned, head_grad


def relay_local(*args):
    n_grp, n_dev = lax.axis_size("grp"), lax.axis_size("dev")
    shard_rows = VOCAB // args[-1].shape[0]
    rows_in, packed, where, slot_info, head, flag = relay_exchange(
        args, n_grp, n_dev, shard_rows // BLOCKS
    )

    def relayed(operands):
        return place_packed(shard_rows, operands[2], operands[1])

    def spread(operands):
        rows, _, _, info = operands
        return place_all(
            shard_rows, rows, info[:, 0].reshape(-1).astype(jnp.int32), info[:, 1].reshape(-1)
        )

    owned = lax.switch(
        flag.reshape(()),
        (relayed, spread, lambda operands: plain_finish(prepare(*args), n_dev)[0]),
        (rows_in, packed, where, slot_info),
    )
    return owned, head.reshape(-1)


def solution(mesh):
    placed = (
        P(("grp", "dev"), None),
        P(("grp", "dev"), None, None),
        P(("grp", "dev"), None),
        P(("grp", "dev")),
        P(),
        P(),
        P(),
        P(),
        P(),
    )
    return jax.shard_map(
        local,
        mesh=mesh,
        in_specs=placed,
        out_specs=(P(("grp", "dev"), None), P(("grp", "dev"))),
        check_vma=False,
    )
```
